512 devices in a mesh: gx: 32 (over z, x_hi, core), gy: 16 (over y, x_lo).
Axes of the slice: x: 4 (x_hi: 2, x_lo: 2; x = x_hi * 2 + x_lo), y: 8, z: 8, core: 2. Of those that a mesh axis runs over, the one named last changes fastest.
Arguments:
- init_re: float32 [1, 1024, 16384], P(None, 'gx', 'gy'), may hold values from -6 to 6
- init_im: float32 [1, 1024, 16384], P(None, 'gx', 'gy'), may hold values from -6 to 6
- onsite: float32 [1024, 16384], P('gx', 'gy'), may hold values from -0.9 to 0.9
- bond_x: int32 [1024, 16384], P('gx', 'gy'), may hold values from 0 to 15
- bond_y: int32 [1024, 16384], P('gx', 'gy'), may hold values from 0 to 15
- hop_table: float32 [16], replicated, may hold values from 1.4 to 1.6
- centre: int32 [1, 2], replicated, may hold values from 0 to 1023
- duration: float32 [1], replicated, may hold values from 0.55 to 0.6
Outputs:
- out_re: float32 [1, 1024, 16384], P(None, 'gx', 'gy')
- out_im: float32 [1, 1024, 16384], P(None, 'gx', 'gy')
- term_norms: float32 [2, 8, 1], replicated
The draws below stay inside these ranges and needn't reach their ends.
All inputs are finite; a program needn't handle non-finite values.
Results may differ from the reference program's by a relative error of at most 0.0003.
Values sent between devices are 32-bit elements; how exact they have to be, the bound alone decides.
No kernel may reach another device: no remote copies, remote signals or barrier semaphores. Data moves between devices by JAX's collectives and lax.ppermute only.
A program may use at most 64 MiB of HBM per device.

```python
import math
import jax
import jax.numpy as jnp
from jax import lax

PACKETS = 1
TERMS = 8
STEPS = 2
CLASSES = 16
NX = 1024
NY = 16384


def draw_onsite(key, part):
    sign_key = jax.random.fold_in(key, 101)
    size_key = jax.random.fold_in(key, 102)
    coin = jax.random.uniform(sign_key, (NX, NY), jnp.float32)
    signs = jnp.where(coin < 0.5, -1.0, 1.0).astype(jnp.float32)
    magnitude = jax.random.uniform(size_key, (NX, NY), jnp.float32, 0.5, 0.9)
    return (signs * magnitude).astype(jnp.float32)


def draw_hop_table(key, part):
    table_key = jax.random.fold_in(key, 201)
    values = jax.random.uniform(table_key, (CLASSES,), jnp.float32, 1.4, 1.6)
    return values.astype(jnp.float32)


def draw_duration(key, part):
    time_key = jax.random.fold_in(key, 301)
    values = jax.random.uniform(time_key, (1,), jnp.float32, 0.55, 0.6)
    return values.astype(jnp.float32)


def place_ends(drawn, own_key, low, largest):
    longest = drawn.shape.index(max(drawn.shape))
    spots = []
    for shift in (0, 1):
        where = [jax.random.randint(jax.random.fold_in(own_key, axis), (), 0, length) for axis, length in enumerate(drawn.shape)]
        where[longest] = (where[longest] + shift) % drawn.shape[longest]
        spots.append(tuple(where))
    return drawn.at[spots[0]].set(low).at[spots[1]].set(largest)


def steps_of(own_key, dims, cuts, least, top_value):
    factor_of, own = 1.0, jax.random.fold_in(own_key, 6)
    for position, blocks in cuts:
        heights = jnp.exp(jax.random.uniform(jax.random.fold_in(own, position), (blocks,), jnp.float32, least / len(cuts), top_value / len(cuts)))
        factor_of = factor_of * jnp.repeat(heights, dims[position] // blocks).reshape([-1 if axis == position else 1 for axis in range(len(dims))])
    return factor_of


def noise(stream_key, dims, spread, bound, split=(), held_as=jnp.bfloat16):
    loudness = steps_of(stream_key, dims, split, -0.22, 0.18) if split else 1.0
    entries = jax.random.normal(stream_key, dims, jnp.float32) * spread * loudness
    return jnp.minimum(jnp.maximum(entries, -bound), bound).astype(held_as)


def setup_inputs(seed: int = 0) -> dict:
    key_list = jax.random.split(jax.random.key(seed), 9)
    init_re = noise(key_list[0], (PACKETS, NX, NY), 1.0, 6.0, ((1, 32), (2, 16)), jnp.float32)
    init_im = noise(key_list[1], (PACKETS, NX, NY), 1.0, 6.0, ((1, 32), (2, 16)), jnp.float32)
    onsite = draw_onsite(jax.random.fold_in(key_list[8], 71), 0)
    bond_x = place_ends(jax.random.randint(key_list[3], (NX, NY), 0, CLASSES), jax.random.fold_in(key_list[3], 1), 0, CLASSES - 1).astype(jnp.int32)
    bond_y = place_ends(jax.random.randint(key_list[4], (NX, NY), 0, CLASSES), jax.random.fold_in(key_list[4], 1), 0, CLASSES - 1).astype(jnp.int32)
    hop_table = draw_hop_table(jax.random.fold_in(key_list[8], 71), 0)
    centre = jax.random.randint(key_list[6], (PACKETS, 2), 0, min(NX, NY)).astype(jnp.int32)
    duration = draw_duration(jax.random.fold_in(key_list[8], 71), 0)
    return dict(init_re=init_re, init_im=init_im, onsite=onsite, bond_x=bond_x, bond_y=bond_y, hop_table=hop_table, centre=centre, duration=duration)


SPECTRAL = 7.5
epsilon = 1e-06

def bessel_weights(duration):
    argument = duration[0] * SPECTRAL
    halved = argument * 0.5
    weights = []
    for degree in range(TERMS):
        series = halved ** degree / math.factorial(degree)
        summed = series
        for counter in range(1, 24):
            series = series * -(halved * halved) / (counter * (counter + degree))
            summed = summed + series
        weights.append(summed if degree == 0 else 2.0 * summed)
    return weights

def rotated(degree, real_part, imag_part):
    quarter = degree % 4
    if quarter == 0:
        return (real_part, imag_part)
    if quarter == 1:
        return (imag_part, -real_part)
    if quarter == 2:
        return (-real_part, -imag_part)
    return (-imag_part, real_part)

def falloff(positions, centres, extent):
    distance = jnp.mod(positions - centres, extent)
    distance = jnp.minimum(distance, extent - distance).astype(jnp.float32)
    return distance * distance * (4.5 / (extent * extent))

def hamiltonian(grid_field, onsite, hop_down, hop_up, hop_right, hop_left):
    result = onsite * grid_field
    result = result - hop_down * jnp.roll(grid_field, -1, 1)
    result = result - hop_up * jnp.roll(grid_field, 1, 1)
    result = result - hop_right * jnp.roll(grid_field, -1, 2)
    result = result - hop_left * jnp.roll(grid_field, 1, 2)
    return result * (1.0 / SPECTRAL)

def reference(init_re, init_im, onsite, bond_x, bond_y, hop_table, centre, duration):
    hop_down = hop_table[bond_x]
    hop_right = hop_table[bond_y]
    hop_up = jnp.roll(hop_down, 1, 0)
    hop_left = jnp.roll(hop_right, 1, 1)
    weights = bessel_weights(duration)
    cell_count = NX * NY
    row_ids = jnp.arange(NX, dtype=jnp.int32)
    col_ids = jnp.arange(NY, dtype=jnp.int32)

    def one_packet(inputs):
        real_init, imag_init, centres = inputs
        row_fall = falloff(row_ids, centres[0], NX)
        col_fall = falloff(col_ids, centres[1], NY)
        envelope = jnp.exp(-(row_fall[:, None] + col_fall[None, :]))
        packet_state = jnp.stack([real_init * envelope, imag_init * envelope])
        norm_rows = []
        for repeat in range(STEPS):
            previous = packet_state
            current = packet_state
            accumulate = weights[0] * packet_state
            norm_list = [jnp.sum(packet_state * packet_state) / cell_count]
            for degree in range(1, TERMS):
                applied = hamiltonian(current, onsite, hop_down, hop_up, hop_right, hop_left)
                following = applied if degree == 1 else 2.0 * applied - previous
                previous, current = (current, following)
                real_rot, imag_rot = rotated(degree, following[0], following[1])
                accumulate = accumulate + weights[degree] * jnp.stack([real_rot, imag_rot])
                norm_list.append(jnp.sum(following * following) / cell_count)
            rescale = lax.rsqrt(jnp.sum(accumulate * accumulate) / cell_count + epsilon)
            packet_state = accumulate * rescale
            norm_rows.append(jnp.stack(norm_list))
        return (packet_state[0], packet_state[1], jnp.stack(norm_rows))
    real_out, imag_out, norm_table = lax.map(one_packet, (init_re, init_im, centre))
    return (real_out, imag_out, jnp.transpose(norm_table, (1, 2, 0)))
```

```python
import functools
import math

import jax
import jax.numpy as jnp
from jax import lax
from jax.experimental import pallas as pl
from jax.experimental.pallas import tpu as pltpu
from jax.sharding import PartitionSpec as P

TERMS = 8
STEPS = 2
SPECTRAL = 7.5
EPSILON = 1e-06
REACH = STEPS * (TERMS - 1)
LANES = 128
GAP = 16
PAD = 8
TOP = 16
FIELDS = 5
VMEM = pltpu.VMEM
SMEM = pltpu.SMEM


def lane_of(shape):
    return lax.broadcasted_iota(jnp.int32, shape, len(shape) - 1)


def falloff(positions, centre, extent):
    distance = positions - centre
    distance = jnp.where(distance < 0, distance + extent, distance)
    distance = jnp.minimum(distance, extent - distance).astype(jnp.float32)
    return jnp.exp(-(distance * distance * (4.5 / (extent * extent))))


def row_envelope(start, count, row_base, centre, extent):
    positions = row_base + start + lax.broadcasted_iota(jnp.int32, (count, LANES), 0)
    return falloff(positions, centre, extent)


def column_envelope(tile, column_base, centre, extent):
    positions = column_base + tile * LANES + lane_of((1, LANES))
    return falloff(positions, centre, extent)


def table_lanes(table_ref, classes):
    lane = lane_of((8, LANES))
    table = jnp.zeros((8, LANES), jnp.float32)
    for entry in range(classes):
        table = jnp.where(lane == entry, table_ref[entry], table)
    return table


def looked_up(table, codes):
    rows = codes.shape[0]
    whole = jnp.concatenate([table] * -(-rows // 8), axis=0)[:rows]
    return jnp.take_along_axis(whole, codes, axis=1)


def bases(rows, cols, gx, gy):
    return lax.axis_index(gx) * rows, lax.axis_index(gy) * cols


def fields_of(refs, table, rows, tile, envelope):
    re_ref, im_ref, onsite_ref, down_ref, right_ref = refs
    cut = (slice(*rows), pl.ds(tile * LANES, LANES))
    return [
        re_ref[0, cut[0], cut[1]] * envelope,
        im_ref[0, cut[0], cut[1]] * envelope,
        onsite_ref[cut],
        looked_up(table, down_ref[cut]),
        looked_up(table, right_ref[cut]),
    ]


def strip_kernel(gx, gy, extents, table_ref, centre_ref, re, im, onsite, down, right, west_ref, east_ref):
    rows, cols = onsite.shape
    row_base, col_base = bases(rows, cols, gx, gy)
    table = table_lanes(table_ref, table_ref.shape[0])
    row_part = row_envelope(0, rows, row_base, centre_ref[0, 0], extents[0])
    lane = lane_of((rows, LANES))
    for last, out_ref in ((False, west_ref), (True, east_ref)):
        tile = cols // LANES - 1 if last else 0
        envelope = row_part * column_envelope(tile, col_base, centre_ref[0, 1], extents[1])
        values = fields_of((re, im, onsite, down, right), table, (0, rows), tile, envelope)
        packed = jnp.zeros((rows, LANES), jnp.float32)
        for index, value in enumerate(values):
            if last:
                moved = pltpu.roll(value, (LANES - GAP * index) % LANES, 1)
                inside = (lane >= LANES - REACH - GAP * index) & (lane < LANES - GAP * index)
            else:
                moved = pltpu.roll(value, GAP * index, 1)
                inside = (lane >= GAP * index) & (lane < GAP * index + REACH)
            packed = jnp.where(inside, moved, packed)
        out_ref[...] = packed


def halo_columns(from_west, from_east, index):
    lane = lane_of(from_west.shape)
    right = pltpu.roll(from_east, (LANES - GAP * index) % LANES, 1)
    left = pltpu.roll(from_west, GAP * index, 1)
    return jnp.where(lane < REACH, right, jnp.where(lane >= LANES - REACH, left, 0.0))


def rows_kernel(gx, gy, extents, table_ref, centre_ref, re, im, onsite, down, right, from_west, from_east, up_ref, down_out_ref):
    rows, cols = onsite.shape
    row_base, col_base = bases(rows, cols, gx, gy)
    table = table_lanes(table_ref, table_ref.shape[0])
    tiles = cols // LANES
    for first, out_ref in ((0, up_ref), (rows - REACH, down_out_ref)):
        row_part = row_envelope(first, REACH, row_base, centre_ref[0, 0], extents[0])
        for tile in range(tiles + 1):
            if tile == tiles:
                west, east = (r[first : first + REACH, :] for r in (from_west, from_east))
                values = [halo_columns(west, east, index) for index in range(FIELDS)]
            else:
                envelope = row_part * column_envelope(tile, col_base, centre_ref[0, 1], extents[1])
                values = fields_of((re, im, onsite, down, right), table, (first, first + REACH), tile, envelope)
            for index, value in enumerate(values):
                out_ref[index * REACH : (index + 1) * REACH, tile * LANES : (tile + 1) * LANES] = value


def bessel_weights(duration):
    halved = jnp.full((8, LANES), duration * (SPECTRAL * 0.5), jnp.float32)
    square = -(halved * halved)
    weights = []
    power = jnp.ones((8, LANES), jnp.float32)
    for degree in range(TERMS):
        series = jnp.ones((8, LANES), jnp.float32)
        for counter in range(23, 0, -1):
            series = 1.0 + series * (square * (1.0 / (counter * (counter + degree))))
        scale = (1.0 if degree == 0 else 2.0) / math.factorial(degree)
        weights.append(series * power * scale)
        power = power * halved
    return weights


def main_kernel(gx, gy, extents, copies, table_ref, centre_ref, duration_ref, re, im, onsite, down, right,
                from_west, from_east, from_up, from_down, out_re, out_im, sums_ref,
                psi, odd, even, total, coeffs, up_left, weight_ref, norm_ref):
    rows, cols = onsite.shape
    tiles = cols // LANES
    row_base, col_base = bases(rows, cols, gx, gy)
    table = table_lanes(table_ref, table_ref.shape[0])
    own = PAD + TOP
    scales = (1.0, 1.0, 2.0 / SPECTRAL, -2.0 / SPECTRAL, -2.0 / SPECTRAL)
    targets = [psi.at[0], psi.at[1], coeffs.at[0], coeffs.at[1], coeffs.at[2]]

    for degree, weight in enumerate(bessel_weights(duration_ref[0])):
        weight_ref[degree] = weight

    row_part = row_envelope(0, rows, row_base, centre_ref[0, 0], extents[0])
    for tile in range(tiles + 1):
        if tile == tiles:
            values = [halo_columns(from_west[...], from_east[...], index) for index in range(FIELDS)]
        else:
            envelope = row_part * column_envelope(tile, col_base, centre_ref[0, 1], extents[1])
            values = fields_of((re, im, onsite, down, right), table, (0, rows), tile, envelope)
        for value, target, scale in zip(values, targets, scales):
            target[tile, own : own + rows, :] = value if scale == 1.0 else value * scale
        for index, (target, scale) in enumerate(zip(targets, scales)):
            for source, start in ((from_up, own - REACH), (from_down, own + rows)):
                value = source[index * REACH : (index + 1) * REACH, tile * LANES : (tile + 1) * LANES]
                target[tile, start : start + REACH, :] = value if scale == 1.0 else value * scale

    lane = lane_of((8, LANES))
    count = rows // 8
    first_core = TOP // 8
    every = list(range(count + 4))

    def west_of(tile):
        return jnp.where(tile == 0, tiles, tile - 1)

    def east_of(tile):
        return jnp.where(tile == tiles, 0, tile + 1)

    def shift_coeffs(tile, carry):
        other = west_of(tile)
        for block in every:
            at = pl.ds(PAD + 8 * block, 8)
            up_left[0, tile, at, :] = coeffs[1, tile, pl.ds(PAD + 8 * block - 1, 8), :]
            joined = jnp.where(lane == LANES - 1, coeffs[2, other, at, :], coeffs[2, tile, at, :])
            up_left[1, tile, at, :] = pltpu.roll(joined, 1, 1)
        return carry

    lax.fori_loop(0, tiles + 1, shift_coeffs, 0)

    def apply(step, degree, current, previous, target):
        level = step * (TERMS - 1) + degree
        blocks = [b for b in every
                  if 8 * (b + 1) - TOP > level - REACH and 8 * b - TOP < rows + REACH - level]
        wanted = [b for b in every
                  if 8 * (b + 1) - TOP > -(REACH - TERMS + 1) and 8 * b - TOP < rows + REACH - TERMS + 1]
        core = list(range(first_core, first_core + count))
        last_step = step == STEPS - 1

        def body(tile, carry):
            before, norm, norm_zero = carry
            west, east = west_of(tile), east_of(tile)
            squares = None
            zero_squares = None
            for block in blocks:
                at = pl.ds(PAD + 8 * block, 8)
                pot, hop_d, hop_r = (coeffs[k, tile, at, :] for k in range(3))
                hop_u, hop_l = (up_left[k, tile, at, :] for k in range(2))
                found = []
                for part in range(2):
                    centre = current[part, tile, at, :]
                    below = current[part, tile, pl.ds(PAD + 8 * block + 1, 8), :]
                    above = current[part, tile, pl.ds(PAD + 8 * block - 1, 8), :]
                    left = pltpu.roll(jnp.where(lane == LANES - 1, current[part, west, at, :], centre), 1, 1)
                    right_ = pltpu.roll(jnp.where(lane == 0, current[part, east, at, :], centre), LANES - 1, 1)
                    applied = (pot * centre + hop_d * below) + (hop_u * above + hop_r * right_) + hop_l * left
                    if degree == 1:
                        following = 0.5 * applied
                    else:
                        following = applied - previous[part, tile, at, :]
                    target[part, tile, at, :] = following
                    found.append(following)
                keep = core if last_step else wanted
                if block in keep:
                    quarter = degree % 4
                    first, second = (found[0], found[1]) if quarter % 2 == 0 else (found[1], found[0])
                    weight = weight_ref[degree]
                    adds = (first * weight, second * weight)
                    signs = {0: (1, 1), 1: (1, -1), 2: (-1, -1), 3: (-1, 1)}[quarter]
                    for part in range(2):
                        if degree == 1:
                            base = current[part, tile, at, :] * weight_ref[0]
                        elif last_step:
                            base = even_total[part, tile, pl.ds(PAD + 8 * block, 8), :]
                        else:
                            base = total[part, tile, at, :]
                        value = base + adds[part] if signs[part] > 0 else base - adds[part]
                        if last_step:
                            even_total[part, tile, at, :] = value
                        else:
                            total[part, tile, at, :] = value
                if block in core:
                    for part in range(2):
                        square = found[part] * found[part]
                        squares = square if squares is None else squares + square
                        if degree == 1:
                            start = current[part, tile, at, :]
                            start = start * start
                            zero_squares = start if zero_squares is None else zero_squares + start
            norm = norm + jnp.where(tile < tiles, squares, 0.0)
            if degree == 1:
                norm_zero = norm_zero + jnp.where(tile < tiles, zero_squares, 0.0)
            return before, norm, norm_zero

        zero = jnp.zeros((8, LANES), jnp.float32)
        _, norm, norm_zero = lax.fori_loop(0, tiles + 1, body, (0, zero, zero))
        norm_ref[step * TERMS + degree] = norm
        if degree == 1:
            norm_ref[step * TERMS] = norm_zero

    even_total = psi
    for step in range(STEPS):
        start = psi if step == 0 else total
        sequence = [start, odd, even]
        apply(step, 1, start, None, odd)
        apply(step, 2, odd, start, even)
        for degree in range(3, TERMS):
            if degree % 2:
                apply(step, degree, even, odd, odd)
            else:
                apply(step, degree, odd, even, even)
        source = total if step < STEPS - 1 else even_total
        square = jnp.zeros((8, LANES), jnp.float32)
        for tile in range(tiles):
            for block in range(first_core, first_core + count):
                for part in range(2):
                    value = source[part, tile, pl.ds(PAD + 8 * block, 8), :]
                    square = square + value * value
                    if step == STEPS - 1:
                        out_ref = (out_re, out_im)[part]
                        out_ref[8 * (block - first_core) : 8 * (block - first_core) + 8, tile * LANES : (tile + 1) * LANES] = value
        norm_ref[STEPS * TERMS + step] = square

    lane_row = lane_of((1, LANES))
    packed = jnp.zeros((1, LANES), jnp.float32)
    for index in range(STEPS * TERMS + STEPS):
        found = jnp.sum(jnp.sum(norm_ref[index], axis=0, keepdims=True), axis=1, keepdims=True)
        packed = jnp.where(lane_row == index, found, packed)
    sums_ref[...] = jnp.broadcast_to(packed, (copies, LANES))


def scale_kernel(cell_count, totals_ref, re_ref, im_ref, out_re, out_im, norms_ref):
    totals = jnp.sum(totals_ref[...], axis=0, keepdims=True) * (1.0 / cell_count)
    lane = lane_of(totals.shape)
    factor = jnp.ones((1, 1), jnp.float32)
    for step in range(STEPS):
        squared = factor * factor
        moved = totals if step == 0 else pltpu.roll(totals, LANES - step * TERMS, 1)
        norms_ref[step] = (moved * squared)[:, :TERMS]
        mean = jnp.sum(jnp.where(lane == STEPS * TERMS + step, totals, 0.0), axis=1, keepdims=True) * squared
        factor = factor * lax.rsqrt(mean + EPSILON)
    out_re[0] = re_ref[...] * factor
    out_im[0] = im_ref[...] * factor


def neighbours(block_low, block_high, axis, count):
    forward = [(i, (i + 1) % count) for i in range(count)]
    backward = [(target, source) for source, target in forward]
    from_previous = lax.ppermute(block_high, axis, forward)
    from_next = lax.ppermute(block_low, axis, backward)
    return from_previous, from_next


def grant(mebibytes):
    return pltpu.CompilerParams(vmem_limit_bytes=mebibytes * 2**20)


def vmem_specs(count):
    return [pl.BlockSpec(memory_space=VMEM)] * count


def per_device(gx, gy, counts, interpret, init_re, init_im, onsite, bond_x, bond_y, hop_table, centre, duration):
    rows, cols = onsite.shape
    extents = (rows * counts[0], cols * counts[1])
    tiles = cols // LANES
    both = gx + gy
    everyone = counts[0] * counts[1]
    smem = [pl.BlockSpec(memory_space=SMEM)]
    local = (init_re, init_im, onsite, bond_x, bond_y)
    shape = lambda *s: jax.ShapeDtypeStruct(s, jnp.float32)
    height = rows + 2 * TOP + 2 * PAD

    west, east = pl.pallas_call(
        functools.partial(strip_kernel, gx, gy, extents),
        out_shape=[shape(rows, LANES)] * 2,
        in_specs=smem * 2 + vmem_specs(5), out_specs=vmem_specs(2), interpret=interpret, name="strips", compiler_params=grant(4),
    )(hop_table, centre, *local)
    from_west, from_east = neighbours(west, east, gy, counts[1])
    packed_rows = -(-FIELDS * REACH // 8) * 8
    up, down = pl.pallas_call(
        functools.partial(rows_kernel, gx, gy, extents),
        out_shape=[shape(packed_rows, cols + LANES)] * 2,
        in_specs=smem * 2 + vmem_specs(7), out_specs=vmem_specs(2), interpret=interpret, name="rows", compiler_params=grant(8),
    )(hop_table, centre, *local, from_west, from_east)
    from_up, from_down = neighbours(up, down, gx, counts[0])
    panel = lambda n: pltpu.VMEM((n, tiles + 1, height, LANES), jnp.float32)
    acc_re, acc_im, sums = pl.pallas_call(
        functools.partial(main_kernel, gx, gy, extents, everyone),
        out_shape=[shape(rows, cols), shape(rows, cols), shape(everyone, LANES)],
        in_specs=smem * 3 + vmem_specs(9), out_specs=vmem_specs(3),
        scratch_shapes=[panel(2), panel(2), panel(2), panel(2), panel(3), panel(2),
                        pltpu.VMEM((TERMS, 8, LANES), jnp.float32),
                        pltpu.VMEM((STEPS * TERMS + STEPS, 8, LANES), jnp.float32)],
        interpret=interpret, name="chebyshev", compiler_params=grant(20),
    )(hop_table, centre, duration, *local, from_west, from_east, from_up, from_down)
    totals = lax.all_to_all(sums, both, 0, 0, tiled=True)
    out_re, out_im, norms = pl.pallas_call(
        functools.partial(scale_kernel, extents[0] * extents[1]),
        out_shape=[shape(1, rows, cols), shape(1, rows, cols), shape(STEPS, 1, TERMS)],
        in_specs=vmem_specs(3), out_specs=vmem_specs(3), interpret=interpret, name="scale", compiler_params=grant(4),
    )(totals, acc_re, acc_im)
    return out_re, out_im, jnp.swapaxes(norms, 1, 2)


def solution(mesh, interpret=False):
    gx, gy = ("gx",), ("gy",)
    counts = (mesh.shape["gx"], mesh.shape["gy"])
    whole, plane = P(None, "gx", "gy"), P("gx", "gy")
    return jax.shard_map(
        functools.partial(per_device, gx, gy, counts, interpret),
        mesh=mesh,
        in_specs=(whole, whole, plane, plane, plane, P(), P(), P()),
        out_specs=(whole, whole, P()),
        check_vma=False,
    )
```

```python
import functools
import math

import jax
import jax.numpy as jnp
from jax import lax
from jax.experimental import pallas as pl
from jax.experimental.pallas import tpu as pltpu
from jax.sharding import PartitionSpec as P

TERMS = 8
STEPS = 2
SPECTRAL = 7.5
EPSILON = 1e-06
REACH = STEPS * (TERMS - 1)
LANES = 128
GAP = 16
PAD = 8
TOP = 16
FIELDS = 5
UNROLL = 9
VMEM = pltpu.VMEM
SMEM = pltpu.SMEM


def lane_of(shape):
    return lax.broadcasted_iota(jnp.int32, shape, len(shape) - 1)


def falloff(positions, centre, extent):
    distance = positions - centre
    distance = jnp.where(distance < 0, distance + extent, distance)
    distance = jnp.minimum(distance, extent - distance).astype(jnp.float32)
    return jnp.exp(-(distance * distance * (4.5 / (extent * extent))))


def row_envelope(start, count, row_base, centre, extent):
    positions = row_base + start + lax.broadcasted_iota(jnp.int32, (count, LANES), 0)
    return falloff(positions, centre, extent)


def column_envelope(tile, column_base, centre, extent):
    positions = column_base + tile * LANES + lane_of((1, LANES))
    return falloff(positions, centre, extent)


def table_lanes(table_ref, classes):
    lane = lane_of((8, LANES))
    table = jnp.zeros((8, LANES), jnp.float32)
    for entry in range(classes):
        table = jnp.where(lane == entry, table_ref[entry], table)
    return table


def looked_up(table, codes):
    rows = codes.shape[0]
    whole = jnp.concatenate([table] * -(-rows // 8), axis=0)[:rows]
    return jnp.take_along_axis(whole, codes, axis=1)


def bases(rows, cols, gx, gy):
    return lax.axis_index(gx) * rows, lax.axis_index(gy) * cols


def fields_kernel(gx, gy, extents, table_hbm, centre_hbm, re, im, onsite, down, right, fields_ref, near_ref, far_ref,
                  table_ref, centre_ref, fine, codes, sems):
    rows, cols = onsite.shape
    copies = [
        (table_hbm, table_ref),
        (centre_hbm, centre_ref),
        (re.at[0], fine.at[0]),
        (im.at[0], fine.at[1]),
        (down, codes.at[0]),
        (right, codes.at[1]),
        (onsite, fields_ref.at[2]),
    ]
    started = [pltpu.make_async_copy(source, target, sems.at[i]) for i, (source, target) in enumerate(copies)]
    for copy in started:
        copy.start()
    for copy in started:
        copy.wait()
    row_base, col_base = bases(rows, cols, gx, gy)
    table = table_lanes(table_ref, table_ref.shape[0])
    row_part = row_envelope(0, rows, row_base, centre_ref[0, 0], extents[0])
    lane = lane_of((rows, LANES))
    tiles = cols // LANES
    packs = []
    for tile in (0, tiles - 1, *range(1, tiles - 1)):
        cut = slice(tile * LANES, (tile + 1) * LANES)
        envelope = row_part * column_envelope(tile, col_base, centre_ref[0, 1], extents[1])
        values = [
            fine[0, :, cut] * envelope,
            fine[1, :, cut] * envelope,
            fields_ref[2, :, cut],
            looked_up(table, codes[0, :, cut]),
            looked_up(table, codes[1, :, cut]),
        ]
        for index in (0, 1, 3, 4):
            fields_ref[index, :, cut] = values[index]
        if 0 < tile < tiles - 1:
            continue
        packed = jnp.zeros((rows, LANES), jnp.float32)
        for index, value in enumerate(values):
            if tile:
                moved = pltpu.roll(value, (LANES - GAP * index) % LANES, 1)
                inside = (lane >= LANES - REACH - GAP * index) & (lane < LANES - GAP * index)
            else:
                moved = pltpu.roll(value, GAP * index, 1)
                inside = (lane >= GAP * index) & (lane < GAP * index + REACH)
            packed = jnp.where(inside, moved, packed)
        packs.append(packed)
    west, east = packs
    odd = lax.rem(lax.axis_index(gy), 2) == 1
    near_ref[...] = jnp.where(odd, west, east)
    far_ref[...] = jnp.where(odd, east, west)


def strips_from(gy, near_ref, far_ref):
    rows = far_ref.shape[0]
    parity = lax.rem(lax.axis_index(gy), 2)
    near = near_ref[pl.ds(pl.multiple_of((1 - parity) * rows, 8), rows), :]
    far = far_ref[...]
    odd = parity == 1
    return jnp.where(odd, near, far), jnp.where(odd, far, near)


def halo_columns(from_west, from_east, index):
    lane = lane_of(from_west.shape)
    right = pltpu.roll(from_east, (LANES - GAP * index) % LANES, 1)
    left = pltpu.roll(from_west, GAP * index, 1)
    return jnp.where(lane < REACH, right, jnp.where(lane >= LANES - REACH, left, 0.0))


def rows_kernel(gx, gy, fields_ref, near_strip, far_strip, near_ref, far_ref):
    _, rows, cols = fields_ref.shape
    from_west, from_east = strips_from(gy, near_strip, far_strip)
    parity = lax.rem(lax.axis_index(gx), 2)

    def fill(first, out_ref):
        west, east = (r[first : first + REACH, :] for r in (from_west, from_east))
        for index in range(FIELDS):
            at = slice(index * REACH, (index + 1) * REACH)
            out_ref[at, cols : cols + LANES] = halo_columns(west, east, index)
            out_ref[at, :cols] = fields_ref[index, first : first + REACH, :]

    @pl.when(parity == 0)
    def _():
        fill(0, far_ref)
        fill(rows - REACH, near_ref)

    @pl.when(parity == 1)
    def _():
        fill(0, near_ref)
        fill(rows - REACH, far_ref)


def bessel_weights(duration):
    halved = jnp.full((8, LANES), duration * (SPECTRAL * 0.5), jnp.float32)
    square = -(halved * halved)
    weights = []
    power = jnp.ones((8, LANES), jnp.float32)
    for degree in range(TERMS):
        series = jnp.ones((8, LANES), jnp.float32)
        for counter in range(23, 0, -1):
            series = 1.0 + series * (square * (1.0 / (counter * (counter + degree))))
        scale = (1.0 if degree == 0 else 2.0) / math.factorial(degree)
        weights.append(series * power * scale)
        power = power * halved
    return weights


def main_kernel(gx, gy, copies, duration_ref, fields_ref,
                near_strip, far_strip, near_rows, far_rows, out_re, out_im, sums_ref,
                psi, odd, even, total, coeffs, up_left, weight_ref, norm_ref):
    _, rows, cols = fields_ref.shape
    tiles = cols // LANES
    own = PAD + TOP
    scales = (1.0, 1.0, 2.0 / SPECTRAL, -2.0 / SPECTRAL, -2.0 / SPECTRAL)
    targets = [psi.at[0], psi.at[1], coeffs.at[0], coeffs.at[1], coeffs.at[2]]

    for degree, weight in enumerate(bessel_weights(duration_ref[0])):
        weight_ref[degree] = weight

    from_west, from_east = strips_from(gy, near_strip, far_strip)
    for index, (target, scale) in enumerate(zip(targets, scales)):
        for tile in range(tiles + 1):
            if tile == tiles:
                value = halo_columns(from_west, from_east, index)
            else:
                value = fields_ref[index, :, tile * LANES : (tile + 1) * LANES]
            target[tile, own : own + rows, :] = value if scale == 1.0 else value * scale

    packed_rows = far_rows.shape[0]

    def place(from_up, from_down):
        for source, base, start in ((*from_up, own - REACH), (*from_down, own + rows)):
            for index, (target, scale) in enumerate(zip(targets, scales)):
                first = base + index * REACH
                for tile in range(tiles + 1):
                    value = source[first : first + REACH, tile * LANES : (tile + 1) * LANES]
                    target[tile, start : start + REACH, :] = value if scale == 1.0 else value * scale

    row_parity = lax.rem(lax.axis_index(gx), 2)

    @pl.when(row_parity == 0)
    def _():
        place((far_rows, 0), (near_rows, packed_rows))

    @pl.when(row_parity == 1)
    def _():
        place((near_rows, 0), (far_rows, 0))

    lane = lane_of((8, LANES))
    count = rows // 8
    first_core = TOP // 8
    every = list(range(count + 4))

    def west_of(tile):
        if isinstance(tile, int):
            return (tile - 1) % (tiles + 1)
        return jnp.where(tile == 0, tiles, tile - 1)

    def east_of(tile):
        if isinstance(tile, int):
            return (tile + 1) % (tiles + 1)
        return jnp.where(tile == tiles, 0, tile + 1)

    def shift_coeffs(tile, carry):
        other = west_of(tile)
        for block in every:
            at = pl.ds(PAD + 8 * block, 8)
            up_left[0, tile, at, :] = coeffs[1, tile, pl.ds(PAD + 8 * block - 1, 8), :]
            joined = jnp.where(lane == LANES - 1, coeffs[2, other, at, :], coeffs[2, tile, at, :])
            up_left[1, tile, at, :] = pltpu.roll(joined, 1, 1)
        return carry

    lax.fori_loop(0, tiles + 1, shift_coeffs, 0)

    def apply(step, degree, current, previous, target):
        level = step * (TERMS - 1) + degree
        blocks = [b for b in every
                  if 8 * (b + 1) - TOP > level - REACH and 8 * b - TOP < rows + REACH - level]
        wanted = [b for b in every
                  if 8 * (b + 1) - TOP > -(REACH - TERMS + 1) and 8 * b - TOP < rows + REACH - TERMS + 1]
        core = list(range(first_core, first_core + count))
        last_step = step == STEPS - 1

        def body(tile, carry):
            before, norm, norm_zero = carry
            west, east = west_of(tile), east_of(tile)
            squares = None
            zero_squares = None
            for block in blocks:
                at = pl.ds(PAD + 8 * block, 8)
                pot, hop_d, hop_r = (coeffs[k, tile, at, :] for k in range(3))
                hop_u, hop_l = (up_left[k, tile, at, :] for k in range(2))
                found = []
                for part in range(2):
                    centre = current[part, tile, at, :]
                    below = current[part, tile, pl.ds(PAD + 8 * block + 1, 8), :]
                    above = current[part, tile, pl.ds(PAD + 8 * block - 1, 8), :]
                    left = pltpu.roll(jnp.where(lane == LANES - 1, current[part, west, at, :], centre), 1, 1)
                    right_ = pltpu.roll(jnp.where(lane == 0, current[part, east, at, :], centre), LANES - 1, 1)
                    applied = (pot * centre + hop_d * below) + (hop_u * above + hop_r * right_) + hop_l * left
                    if degree == 1:
                        following = 0.5 * applied
                    else:
                        following = applied - previous[part, tile, at, :]
                    target[part, tile, at, :] = following
                    found.append(following)
                keep = core if last_step else wanted
                if block in keep:
                    quarter = degree % 4
                    first, second = (found[0], found[1]) if quarter % 2 == 0 else (found[1], found[0])
                    weight = weight_ref[degree]
                    adds = (first * weight, second * weight)
                    signs = {0: (1, 1), 1: (1, -1), 2: (-1, -1), 3: (-1, 1)}[quarter]
                    for part in range(2):
                        if degree == 1:
                            base = current[part, tile, at, :] * weight_ref[0]
                        elif last_step:
                            base = even_total[part, tile, pl.ds(PAD + 8 * block, 8), :]
                        else:
                            base = total[part, tile, at, :]
                        value = base + adds[part] if signs[part] > 0 else base - adds[part]
                        if last_step:
                            even_total[part, tile, at, :] = value
                        else:
                            total[part, tile, at, :] = value
                if block in core:
                    for part in range(2):
                        square = found[part] * found[part]
                        squares = square if squares is None else squares + square
                        if degree == 1:
                            start = current[part, tile, at, :]
                            start = start * start
                            zero_squares = start if zero_squares is None else zero_squares + start
            if not isinstance(tile, int):
                squares = jnp.where(tile < tiles, squares, 0.0)
                if degree == 1:
                    zero_squares = jnp.where(tile < tiles, zero_squares, 0.0)
            if not isinstance(tile, int) or tile < tiles:
                norm = norm + squares
                if degree == 1:
                    norm_zero = norm_zero + zero_squares
            return before, norm, norm_zero

        zero = jnp.zeros((8, LANES), jnp.float32)
        carry = (0, zero, zero)
        if UNROLL > tiles:
            for tile in range(tiles + 1):
                carry = body(tile, carry)
        else:
            def group(index, carry):
                for offset in range(UNROLL):
                    carry = body(index * UNROLL + offset, carry)
                return carry

            carry = lax.fori_loop(0, (tiles + 1) // UNROLL, group, carry)
        _, norm, norm_zero = carry
        norm_ref[step * TERMS + degree] = norm
        if degree == 1:
            norm_ref[step * TERMS] = norm_zero

    even_total = psi
    for step in range(STEPS):
        start = psi if step == 0 else total
        sequence = [start, odd, even]
        apply(step, 1, start, None, odd)
        apply(step, 2, odd, start, even)
        for degree in range(3, TERMS):
            if degree % 2:
                apply(step, degree, even, odd, odd)
            else:
                apply(step, degree, odd, even, even)
        source = total if step < STEPS - 1 else even_total
        square = jnp.zeros((8, LANES), jnp.float32)
        for tile in range(tiles):
            for block in range(first_core, first_core + count):
                for part in range(2):
                    value = source[part, tile, pl.ds(PAD + 8 * block, 8), :]
                    square = square + value * value
                    if step == STEPS - 1:
                        out_ref = (out_re, out_im)[part]
                        out_ref[8 * (block - first_core) : 8 * (block - first_core) + 8, tile * LANES : (tile + 1) * LANES] = value
        norm_ref[STEPS * TERMS + step] = square

    lane_row = lane_of((1, LANES))
    packed = jnp.zeros((1, LANES), jnp.float32)
    for index in range(STEPS * TERMS + STEPS):
        found = jnp.sum(jnp.sum(norm_ref[index], axis=0, keepdims=True), axis=1, keepdims=True)
        packed = jnp.where(lane_row == index, found, packed)
    sums_ref[...] = jnp.broadcast_to(packed, (copies, LANES))


def scale_kernel(cell_count, totals_ref, re_ref, im_ref, out_re, out_im, norms_ref):
    totals = jnp.sum(totals_ref[...], axis=0, keepdims=True) * (1.0 / cell_count)
    lane = lane_of(totals.shape)
    factor = jnp.ones((1, 1), jnp.float32)
    for step in range(STEPS):
        squared = factor * factor
        moved = totals if step == 0 else pltpu.roll(totals, LANES - step * TERMS, 1)
        norms_ref[step] = (moved * squared)[:, :TERMS]
        mean = jnp.sum(jnp.where(lane == STEPS * TERMS + step, totals, 0.0), axis=1, keepdims=True) * squared
        factor = factor * lax.rsqrt(mean + EPSILON)
    out_re[0] = re_ref[...] * factor
    out_im[0] = im_ref[...] * factor


def far_pairs(count):
    pairs = [(i, (i + 1) % count) for i in range(1, count, 2)]
    return pairs + [(target, source) for source, target in pairs]


def near_pairs(count):
    return [[i, i + 1] for i in range(0, count, 2)]


def swapped(near, far, axis, count):
    from_far = lax.ppermute(far, axis, far_pairs(count))
    from_near = lax.all_gather(near, axis, axis=0, tiled=True, axis_index_groups=near_pairs(count))
    return from_near, from_far


FIELDS_PARAMS = pltpu.CompilerParams(vmem_limit_bytes=20 * 2**20)


def grant(mebibytes):
    return pltpu.CompilerParams(vmem_limit_bytes=mebibytes * 2**20)


def vmem_specs(count):
    return [pl.BlockSpec(memory_space=VMEM)] * count


def per_device(gx, gy, counts, init_re, init_im, onsite, bond_x, bond_y, hop_table, centre, duration):
    rows, cols = onsite.shape
    extents = (rows * counts[0], cols * counts[1])
    tiles = cols // LANES
    both = gx + gy
    everyone = counts[0] * counts[1]
    smem = [pl.BlockSpec(memory_space=SMEM)]
    local = (init_re, init_im, onsite, bond_x, bond_y)
    shape = lambda *s: jax.ShapeDtypeStruct(s, jnp.float32)
    height = rows + 2 * TOP + 2 * PAD

    hbm = [pl.BlockSpec(memory_space=pltpu.HBM)]
    fields, near, far = pl.pallas_call(
        functools.partial(fields_kernel, gx, gy, extents),
        out_shape=[shape(FIELDS, rows, cols), shape(rows, LANES), shape(rows, LANES)],
        in_specs=hbm * 7, out_specs=vmem_specs(3),
        scratch_shapes=[SMEM(hop_table.shape, jnp.float32), SMEM(centre.shape, jnp.int32), VMEM((2, rows, cols), jnp.float32),
                        VMEM((2, rows, cols), jnp.int32), pltpu.SemaphoreType.DMA((7,))],
        name="fields", compiler_params=FIELDS_PARAMS,
    )(*(pltpu.with_memory_space_constraint(x, pltpu.HBM) for x in (hop_table, centre, *local)))
    near_strip, far_strip = swapped(near, far, gy[0], counts[1])
    packed_rows = -(-FIELDS * REACH // 8) * 8
    near, far = pl.pallas_call(
        functools.partial(rows_kernel, gx, gy),
        out_shape=[shape(packed_rows, cols + LANES)] * 2,
        in_specs=vmem_specs(3), out_specs=vmem_specs(2), name="rows", compiler_params=grant(8),
    )(fields, near_strip, far_strip)
    near_rows, far_rows = swapped(near, far, gx[0], counts[0])
    panel = lambda n: pltpu.VMEM((n, tiles + 1, height, LANES), jnp.float32)
    acc_re, acc_im, sums = pl.pallas_call(
        functools.partial(main_kernel, gx, gy, everyone),
        out_shape=[shape(rows, cols), shape(rows, cols), shape(everyone, LANES)],
        in_specs=smem + vmem_specs(5), out_specs=vmem_specs(3),
        scratch_shapes=[panel(2), panel(2), panel(2), panel(2), panel(3), panel(2),
                        pltpu.VMEM((TERMS, 8, LANES), jnp.float32),
                        pltpu.VMEM((STEPS * TERMS + STEPS, 8, LANES), jnp.float32)],
        name="chebyshev", compiler_params=grant(20),
    )(duration, fields, near_strip, far_strip, near_rows, far_rows)
    totals = lax.all_to_all(sums, both, 0, 0, tiled=True)
    out_re, out_im, norms = pl.pallas_call(
        functools.partial(scale_kernel, extents[0] * extents[1]),
        out_shape=[shape(1, rows, cols), shape(1, rows, cols), shape(STEPS, 1, TERMS)],
        in_specs=vmem_specs(3), out_specs=vmem_specs(3), name="scale", compiler_params=grant(4),
    )(totals, acc_re, acc_im)
    return out_re, out_im, jnp.swapaxes(norms, 1, 2)


def solution(mesh):
    gx, gy = ("gx",), ("gy",)
    counts = (mesh.shape["gx"], mesh.shape["gy"])
    whole, plane = P(None, "gx", "gy"), P("gx", "gy")
    return jax.shard_map(
        functools.partial(per_device, gx, gy, counts),
        mesh=mesh,
        in_specs=(whole, whole, plane, plane, plane, P(), P(), P()),
        out_specs=(whole, whole, P()),
        check_vma=False,
    )
```

```python
import functools
import math

import jax
import jax.numpy as jnp
from jax import lax
from jax.experimental import pallas as pl
from jax.experimental.pallas import tpu as pltpu
from jax.sharding import PartitionSpec as P

TERMS = 8
STEPS = 2
SPECTRAL = 7.5
EPSILON = 1e-06
REACH = STEPS * (TERMS - 1)
LANES = 128
GAP = 16
PAD = 8
TOP = 16
FIELDS = 5
UNROLL = 9
VMEM = pltpu.VMEM
SMEM = pltpu.SMEM


def lane_of(shape):
    return lax.broadcasted_iota(jnp.int32, shape, len(shape) - 1)


def falloff(positions, centre, extent):
    distance = positions - centre
    distance = jnp.where(distance < 0, distance + extent, distance)
    distance = jnp.minimum(distance, extent - distance).astype(jnp.float32)
    return jnp.exp(-(distance * distance * (4.5 / (extent * extent))))


def row_envelope(start, count, row_base, centre, extent):
    positions = row_base + start + lax.broadcasted_iota(jnp.int32, (count, LANES), 0)
    return falloff(positions, centre, extent)


def column_envelope(tile, column_base, centre, extent):
    positions = column_base + tile * LANES + lane_of((1, LANES))
    return falloff(positions, centre, extent)


def table_lanes(table_ref, classes):
    lane = lane_of((8, LANES))
    table = jnp.zeros((8, LANES), jnp.float32)
    for entry in range(classes):
        table = jnp.where(lane == entry, table_ref[entry], table)
    return table


def looked_up(table, codes):
    rows = codes.shape[0]
    whole = jnp.concatenate([table] * -(-rows // 8), axis=0)[:rows]
    return jnp.take_along_axis(whole, codes, axis=1)


def bases(rows, cols, gx, gy):
    return lax.axis_index(gx) * rows, lax.axis_index(gy) * cols


def fields_kernel(gx, gy, extents, table_hbm, centre_hbm, re, im, onsite, down, right, fields_ref, near_ref, far_ref, far_rows_ref,
                  table_ref, centre_ref, fine, codes, sems):
    rows, cols = onsite.shape
    copies = [
        (table_hbm, table_ref),
        (centre_hbm, centre_ref),
        (re.at[0], fine.at[0]),
        (im.at[0], fine.at[1]),
        (down, codes.at[0]),
        (right, codes.at[1]),
        (onsite, fields_ref.at[2]),
    ]
    started = [pltpu.make_async_copy(source, target, sems.at[i]) for i, (source, target) in enumerate(copies)]
    for copy in started:
        copy.start()
    for copy in started:
        copy.wait()
    row_base, col_base = bases(rows, cols, gx, gy)
    table = table_lanes(table_ref, table_ref.shape[0])
    row_part = row_envelope(0, rows, row_base, centre_ref[0, 0], extents[0])
    lane = lane_of((rows, LANES))
    tiles = cols // LANES
    packs = []
    for tile in (0, tiles - 1, *range(1, tiles - 1)):
        cut = slice(tile * LANES, (tile + 1) * LANES)
        envelope = row_part * column_envelope(tile, col_base, centre_ref[0, 1], extents[1])
        values = [
            fine[0, :, cut] * envelope,
            fine[1, :, cut] * envelope,
            fields_ref[2, :, cut],
            looked_up(table, codes[0, :, cut]),
            looked_up(table, codes[1, :, cut]),
        ]
        for index in (0, 1, 3, 4):
            fields_ref[index, :, cut] = values[index]
        if 0 < tile < tiles - 1:
            continue
        packed = jnp.zeros((rows, LANES), jnp.float32)
        for index, value in enumerate(values):
            if tile:
                moved = pltpu.roll(value, (LANES - GAP * index) % LANES, 1)
                inside = (lane >= LANES - REACH - GAP * index) & (lane < LANES - GAP * index)
            else:
                moved = pltpu.roll(value, GAP * index, 1)
                inside = (lane >= GAP * index) & (lane < GAP * index + REACH)
            packed = jnp.where(inside, moved, packed)
        packs.append(packed)
    west, east = packs
    odd = lax.rem(lax.axis_index(gy), 2) == 1
    near_ref[...] = jnp.where(odd, west, east)
    far_ref[...] = jnp.where(odd, east, west)
    row_parity = lax.rem(lax.axis_index(gx), 2)
    for parity, first in ((0, 0), (1, rows - REACH)):

        @pl.when(row_parity == parity)
        def _(first=first):
            for index in range(FIELDS):
                far_rows_ref[index * REACH : (index + 1) * REACH, :] = fields_ref[index, first : first + REACH, :]


def strips_from(gy, near_ref, far_ref):
    rows = far_ref.shape[0]
    parity = lax.rem(lax.axis_index(gy), 2)
    near = near_ref[pl.ds(pl.multiple_of((1 - parity) * rows, 8), rows), :]
    far = far_ref[...]
    odd = parity == 1
    return jnp.where(odd, near, far), jnp.where(odd, far, near)


def halo_columns(from_west, from_east, index):
    lane = lane_of(from_west.shape)
    right = pltpu.roll(from_east, (LANES - GAP * index) % LANES, 1)
    left = pltpu.roll(from_west, GAP * index, 1)
    return jnp.where(lane < REACH, right, jnp.where(lane >= LANES - REACH, left, 0.0))


def rows_kernel(gx, gy, fields_ref, near_strip, far_strip, near_ref, corner_ref):
    _, rows, cols = fields_ref.shape
    from_west, from_east = strips_from(gy, near_strip, far_strip)
    parity = lax.rem(lax.axis_index(gx), 2)

    def fill(near_first, far_first):
        for index in range(FIELDS):
            at = slice(index * REACH, (index + 1) * REACH)
            cut = slice(near_first, near_first + REACH)
            near_ref[at, cols : cols + LANES] = halo_columns(from_west[cut], from_east[cut], index)
            near_ref[at, :cols] = fields_ref[index, cut, :]
            cut = slice(far_first, far_first + REACH)
            corner_ref[at, :] = halo_columns(from_west[cut], from_east[cut], index)

    @pl.when(parity == 0)
    def _():
        fill(rows - REACH, 0)

    @pl.when(parity == 1)
    def _():
        fill(0, rows - REACH)


def bessel_weights(duration):
    halved = jnp.full((8, LANES), duration * (SPECTRAL * 0.5), jnp.float32)
    square = -(halved * halved)
    weights = []
    power = jnp.ones((8, LANES), jnp.float32)
    for degree in range(TERMS):
        series = jnp.ones((8, LANES), jnp.float32)
        for counter in range(23, 0, -1):
            series = 1.0 + series * (square * (1.0 / (counter * (counter + degree))))
        scale = (1.0 if degree == 0 else 2.0) / math.factorial(degree)
        weights.append(series * power * scale)
        power = power * halved
    return weights


def main_kernel(gx, gy, copies, duration_ref, fields_ref,
                near_strip, far_strip, near_rows, far_rows, far_corner, out_re, out_im, sums_ref,
                psi, odd, even, total, coeffs, up_left, weight_ref, norm_ref):
    _, rows, cols = fields_ref.shape
    tiles = cols // LANES
    own = PAD + TOP
    scales = (1.0, 1.0, 2.0 / SPECTRAL, -2.0 / SPECTRAL, -2.0 / SPECTRAL)
    targets = [psi.at[0], psi.at[1], coeffs.at[0], coeffs.at[1], coeffs.at[2]]

    for degree, weight in enumerate(bessel_weights(duration_ref[0])):
        weight_ref[degree] = weight

    from_west, from_east = strips_from(gy, near_strip, far_strip)
    for index, (target, scale) in enumerate(zip(targets, scales)):
        for tile in range(tiles + 1):
            if tile == tiles:
                value = halo_columns(from_west, from_east, index)
            else:
                value = fields_ref[index, :, tile * LANES : (tile + 1) * LANES]
            target[tile, own : own + rows, :] = value if scale == 1.0 else value * scale

    packed_rows = far_rows.shape[0]

    def place(from_up, from_down):
        for source, base, start in ((*from_up, own - REACH), (*from_down, own + rows)):
            for index, (target, scale) in enumerate(zip(targets, scales)):
                first = base + index * REACH
                for tile in range(tiles + 1):
                    if tile == tiles and source is far_rows:
                        value = far_corner[first : first + REACH, :]
                    else:
                        value = source[first : first + REACH, tile * LANES : (tile + 1) * LANES]
                    target[tile, start : start + REACH, :] = value if scale == 1.0 else value * scale

    row_parity = lax.rem(lax.axis_index(gx), 2)

    @pl.when(row_parity == 0)
    def _():
        place((far_rows, 0), (near_rows, packed_rows))

    @pl.when(row_parity == 1)
    def _():
        place((near_rows, 0), (far_rows, 0))

    lane = lane_of((8, LANES))
    count = rows // 8
    first_core = TOP // 8
    every = list(range(count + 4))

    def west_of(tile):
        if isinstance(tile, int):
            return (tile - 1) % (tiles + 1)
        return jnp.where(tile == 0, tiles, tile - 1)

    def east_of(tile):
        if isinstance(tile, int):
            return (tile + 1) % (tiles + 1)
        return jnp.where(tile == tiles, 0, tile + 1)

    def shift_coeffs(tile, carry):
        other = west_of(tile)
        for block in every:
            at = pl.ds(PAD + 8 * block, 8)
            up_left[0, tile, at, :] = coeffs[1, tile, pl.ds(PAD + 8 * block - 1, 8), :]
            joined = jnp.where(lane == LANES - 1, coeffs[2, other, at, :], coeffs[2, tile, at, :])
            up_left[1, tile, at, :] = pltpu.roll(joined, 1, 1)
        return carry

    lax.fori_loop(0, tiles + 1, shift_coeffs, 0)

    def apply(step, degree, current, previous, target):
        level = step * (TERMS - 1) + degree
        blocks = [b for b in every
                  if 8 * (b + 1) - TOP > level - REACH and 8 * b - TOP < rows + REACH - level]
        wanted = [b for b in every
                  if 8 * (b + 1) - TOP > -(REACH - TERMS + 1) and 8 * b - TOP < rows + REACH - TERMS + 1]
        core = list(range(first_core, first_core + count))
        last_step = step == STEPS - 1

        def body(tile, carry):
            before, norm, norm_zero = carry
            west, east = west_of(tile), east_of(tile)
            squares = None
            zero_squares = None
            for block in blocks:
                at = pl.ds(PAD + 8 * block, 8)
                pot, hop_d, hop_r = (coeffs[k, tile, at, :] for k in range(3))
                hop_u, hop_l = (up_left[k, tile, at, :] for k in range(2))
                found = []
                for part in range(2):
                    centre = current[part, tile, at, :]
                    below = current[part, tile, pl.ds(PAD + 8 * block + 1, 8), :]
                    above = current[part, tile, pl.ds(PAD + 8 * block - 1, 8), :]
                    left = pltpu.roll(jnp.where(lane == LANES - 1, current[part, west, at, :], centre), 1, 1)
                    right_ = pltpu.roll(jnp.where(lane == 0, current[part, east, at, :], centre), LANES - 1, 1)
                    applied = (pot * centre + hop_d * below) + (hop_u * above + hop_r * right_) + hop_l * left
                    if degree == 1:
                        following = 0.5 * applied
                    else:
                        following = applied - previous[part, tile, at, :]
                    target[part, tile, at, :] = following
                    found.append(following)
                keep = core if last_step else wanted
                if block in keep:
                    quarter = degree % 4
                    first, second = (found[0], found[1]) if quarter % 2 == 0 else (found[1], found[0])
                    weight = weight_ref[degree]
                    adds = (first * weight, second * weight)
                    signs = {0: (1, 1), 1: (1, -1), 2: (-1, -1), 3: (-1, 1)}[quarter]
                    for part in range(2):
                        if degree == 1:
                            base = current[part, tile, at, :] * weight_ref[0]
                        elif last_step:
                            base = even_total[part, tile, pl.ds(PAD + 8 * block, 8), :]
                        else:
                            base = total[part, tile, at, :]
                        value = base + adds[part] if signs[part] > 0 else base - adds[part]
                        if last_step:
                            even_total[part, tile, at, :] = value
                        else:
                            total[part, tile, at, :] = value
                if block in core:
                    for part in range(2):
                        square = found[part] * found[part]
                        squares = square if squares is None else squares + square
                        if degree == 1:
                            start = current[part, tile, at, :]
                            start = start * start
                            zero_squares = start if zero_squares is None else zero_squares + start
            if not isinstance(tile, int):
                squares = jnp.where(tile < tiles, squares, 0.0)
                if degree == 1:
                    zero_squares = jnp.where(tile < tiles, zero_squares, 0.0)
            if not isinstance(tile, int) or tile < tiles:
                norm = norm + squares
                if degree == 1:
                    norm_zero = norm_zero + zero_squares
            return before, norm, norm_zero

        zero = jnp.zeros((8, LANES), jnp.float32)
        carry = (0, zero, zero)
        if UNROLL > tiles:
            for tile in range(tiles + 1):
                carry = body(tile, carry)
        else:
            def group(index, carry):
                for offset in range(UNROLL):
                    carry = body(index * UNROLL + offset, carry)
                return carry

            carry = lax.fori_loop(0, (tiles + 1) // UNROLL, group, carry)
        _, norm, norm_zero = carry
        norm_ref[step * TERMS + degree] = norm
        if degree == 1:
            norm_ref[step * TERMS] = norm_zero

    even_total = psi
    for step in range(STEPS):
        start = psi if step == 0 else total
        sequence = [start, odd, even]
        apply(step, 1, start, None, odd)
        apply(step, 2, odd, start, even)
        for degree in range(3, TERMS):
            if degree % 2:
                apply(step, degree, even, odd, odd)
            else:
                apply(step, degree, odd, even, even)
        source = total if step < STEPS - 1 else even_total
        square = jnp.zeros((8, LANES), jnp.float32)
        for tile in range(tiles):
            for block in range(first_core, first_core + count):
                for part in range(2):
                    value = source[part, tile, pl.ds(PAD + 8 * block, 8), :]
                    square = square + value * value
                    if step == STEPS - 1:
                        out_ref = (out_re, out_im)[part]
                        out_ref[8 * (block - first_core) : 8 * (block - first_core) + 8, tile * LANES : (tile + 1) * LANES] = value
        norm_ref[STEPS * TERMS + step] = square

    lane_row = lane_of((1, LANES))
    packed = jnp.zeros((1, LANES), jnp.float32)
    for index in range(STEPS * TERMS + STEPS):
        found = jnp.sum(jnp.sum(norm_ref[index], axis=0, keepdims=True), axis=1, keepdims=True)
        packed = jnp.where(lane_row == index, found, packed)
    sums_ref[...] = jnp.broadcast_to(packed, (copies, LANES))


def scale_kernel(cell_count, totals_ref, re_ref, im_ref, out_re, out_im, norms_ref):
    totals = jnp.sum(totals_ref[...], axis=0, keepdims=True) * (1.0 / cell_count)
    lane = lane_of(totals.shape)
    factor = jnp.ones((1, 1), jnp.float32)
    for step in range(STEPS):
        squared = factor * factor
        moved = totals if step == 0 else pltpu.roll(totals, LANES - step * TERMS, 1)
        norms_ref[step] = (moved * squared)[:, :TERMS]
        mean = jnp.sum(jnp.where(lane == STEPS * TERMS + step, totals, 0.0), axis=1, keepdims=True) * squared
        factor = factor * lax.rsqrt(mean + EPSILON)
    out_re[0] = re_ref[...] * factor
    out_im[0] = im_ref[...] * factor


def far_pairs(count):
    pairs = [(i, (i + 1) % count) for i in range(1, count, 2)]
    return pairs + [(target, source) for source, target in pairs]


def near_pairs(count):
    return [[i, i + 1] for i in range(0, count, 2)]


def from_far_one(value, axis, count):
    return lax.ppermute(value, axis, far_pairs(count))


def from_near_one(value, axis, count):
    return lax.all_gather(value, axis, axis=0, tiled=True, axis_index_groups=near_pairs(count))


FIELDS_PARAMS = pltpu.CompilerParams(vmem_limit_bytes=20 * 2**20)


def grant(mebibytes):
    return pltpu.CompilerParams(vmem_limit_bytes=mebibytes * 2**20)


def vmem_specs(count):
    return [pl.BlockSpec(memory_space=VMEM)] * count


def per_device(gx, gy, counts, init_re, init_im, onsite, bond_x, bond_y, hop_table, centre, duration):
    rows, cols = onsite.shape
    extents = (rows * counts[0], cols * counts[1])
    tiles = cols // LANES
    both = gx + gy
    everyone = counts[0] * counts[1]
    smem = [pl.BlockSpec(memory_space=SMEM)]
    local = (init_re, init_im, onsite, bond_x, bond_y)
    shape = lambda *s: jax.ShapeDtypeStruct(s, jnp.float32)
    height = rows + 2 * TOP + 2 * PAD

    hbm = [pl.BlockSpec(memory_space=pltpu.HBM)]
    packed_rows = -(-FIELDS * REACH // 8) * 8
    fields, near, far, far_main = pl.pallas_call(
        functools.partial(fields_kernel, gx, gy, extents),
        out_shape=[shape(FIELDS, rows, cols), shape(rows, LANES), shape(rows, LANES), shape(packed_rows, cols)],
        in_specs=hbm * 7, out_specs=vmem_specs(4),
        scratch_shapes=[SMEM(hop_table.shape, jnp.float32), SMEM(centre.shape, jnp.int32), VMEM((2, rows, cols), jnp.float32),
                        VMEM((2, rows, cols), jnp.int32), pltpu.SemaphoreType.DMA((7,))],
        name="fields", compiler_params=FIELDS_PARAMS,
    )(*(pltpu.with_memory_space_constraint(x, pltpu.HBM) for x in (hop_table, centre, *local)))
    far_rows = from_far_one(far_main, gx[0], counts[0])
    far_strip = from_far_one(far, gy[0], counts[1])
    near_strip = from_near_one(near, gy[0], counts[1])
    near, corner = pl.pallas_call(
        functools.partial(rows_kernel, gx, gy),
        out_shape=[shape(packed_rows, cols + LANES), shape(packed_rows, LANES)],
        in_specs=vmem_specs(3), out_specs=vmem_specs(2), name="rows", compiler_params=grant(8),
    )(fields, near_strip, far_strip)
    far_corner = from_far_one(corner, gx[0], counts[0])
    near_rows = from_near_one(near, gx[0], counts[0])
    panel = lambda n: pltpu.VMEM((n, tiles + 1, height, LANES), jnp.float32)
    acc_re, acc_im, sums = pl.pallas_call(
        functools.partial(main_kernel, gx, gy, everyone),
        out_shape=[shape(rows, cols), shape(rows, cols), shape(everyone, LANES)],
        in_specs=smem + vmem_specs(6), out_specs=vmem_specs(3),
        scratch_shapes=[panel(2), panel(2), panel(2), panel(2), panel(3), panel(2),
                        pltpu.VMEM((TERMS, 8, LANES), jnp.float32),
                        pltpu.VMEM((STEPS * TERMS + STEPS, 8, LANES), jnp.float32)],
        name="chebyshev", compiler_params=grant(20),
    )(duration, fields, near_strip, far_strip, near_rows, far_rows, far_corner)
    totals = lax.all_to_all(sums, both, 0, 0, tiled=True)
    out_re, out_im, norms = pl.pallas_call(
        functools.partial(scale_kernel, extents[0] * extents[1]),
        out_shape=[shape(1, rows, cols), shape(1, rows, cols), shape(STEPS, 1, TERMS)],
        in_specs=vmem_specs(3), out_specs=vmem_specs(3), name="scale", compiler_params=grant(4),
    )(totals, acc_re, acc_im)
    return out_re, out_im, jnp.swapaxes(norms, 1, 2)


def solution(mesh):
    gx, gy = ("gx",), ("gy",)
    counts = (mesh.shape["gx"], mesh.shape["gy"])
    whole, plane = P(None, "gx", "gy"), P("gx", "gy")
    return jax.shard_map(
        functools.partial(per_device, gx, gy, counts),
        mesh=mesh,
        in_specs=(whole, whole, plane, plane, plane, P(), P(), P()),
        out_specs=(whole, whole, P()),
        check_vma=False,
    )
```

```python
import functools
import math

import jax
import jax.numpy as jnp
from jax import lax
from jax.experimental import pallas as pl
from jax.experimental.pallas import tpu as pltpu
from jax.sharding import Mesh
from jax.sharding import PartitionSpec as P

TERMS = 8
STEPS = 2
SPECTRAL = 7.5
EPSILON = 1e-06
REACH = STEPS * (TERMS - 1)
LANES = 128
GAP = 16
PAD = 8
TOP = 16
FIELDS = 5
UNROLL = 9
VMEM = pltpu.VMEM
SMEM = pltpu.SMEM


def lane_of(shape):
    return lax.broadcasted_iota(jnp.int32, shape, len(shape) - 1)


def falloff(positions, centre, extent):
    distance = positions - centre
    distance = jnp.where(distance < 0, distance + extent, distance)
    distance = jnp.minimum(distance, extent - distance).astype(jnp.float32)
    return jnp.exp(-(distance * distance * (4.5 / (extent * extent))))


def row_envelope(start, count, row_base, centre, extent):
    positions = row_base + start + lax.broadcasted_iota(jnp.int32, (count, LANES), 0)
    return falloff(positions, centre, extent)


def column_envelope(tile, column_base, centre, extent):
    positions = column_base + tile * LANES + lane_of((1, LANES))
    return falloff(positions, centre, extent)


def table_lanes(table_ref, classes):
    lane = lane_of((8, LANES))
    table = jnp.zeros((8, LANES), jnp.float32)
    for entry in range(classes):
        table = jnp.where(lane == entry, table_ref[entry], table)
    return table


def looked_up(table, codes):
    rows = codes.shape[0]
    whole = jnp.concatenate([table] * -(-rows // 8), axis=0)[:rows]
    return jnp.take_along_axis(whole, codes, axis=1)


def bases(rows, cols, gx, gy):
    return lax.axis_index(gx) * rows, lax.axis_index(gy) * cols


def fields_kernel(gx, gy, extents, table_hbm, centre_hbm, re, im, onsite, down, right, fields_ref, near_ref, far_ref, far_rows_ref,
                  table_ref, centre_ref, fine, codes, sems):
    rows, cols = onsite.shape
    copies = [
        (table_hbm, table_ref),
        (centre_hbm, centre_ref),
        (re.at[0], fine.at[0]),
        (im.at[0], fine.at[1]),
        (down, codes.at[0]),
        (right, codes.at[1]),
        (onsite, fields_ref.at[2]),
    ]
    started = [pltpu.make_async_copy(source, target, sems.at[i]) for i, (source, target) in enumerate(copies)]
    for copy in started:
        copy.start()
    for copy in started:
        copy.wait()
    row_base, col_base = bases(rows, cols, gx, gy)
    table = table_lanes(table_ref, table_ref.shape[0])
    row_part = row_envelope(0, rows, row_base, centre_ref[0, 0], extents[0])
    lane = lane_of((rows, LANES))
    tiles = cols // LANES
    packs = []
    for tile in (0, tiles - 1, *range(1, tiles - 1)):
        cut = slice(tile * LANES, (tile + 1) * LANES)
        envelope = row_part * column_envelope(tile, col_base, centre_ref[0, 1], extents[1])
        values = [
            fine[0, :, cut] * envelope,
            fine[1, :, cut] * envelope,
            fields_ref[2, :, cut],
            looked_up(table, codes[0, :, cut]),
            looked_up(table, codes[1, :, cut]),
        ]
        for index in (0, 1, 3, 4):
            fields_ref[index, :, cut] = values[index]
        if 0 < tile < tiles - 1:
            continue
        packed = jnp.zeros((rows, LANES), jnp.float32)
        for index, value in enumerate(values):
            if tile:
                moved = pltpu.roll(value, (LANES - GAP * index) % LANES, 1)
                inside = (lane >= LANES - REACH - GAP * index) & (lane < LANES - GAP * index)
            else:
                moved = pltpu.roll(value, GAP * index, 1)
                inside = (lane >= GAP * index) & (lane < GAP * index + REACH)
            packed = jnp.where(inside, moved, packed)
        packs.append(packed)
    west, east = packs
    odd = lax.rem(lax.axis_index(gy), 2) == 1
    near_ref[...] = jnp.where(odd, west, east)
    far_ref[...] = jnp.where(odd, east, west)
    row_parity = lax.rem(lax.axis_index(gx), 2)
    for parity, first in ((0, 0), (1, rows - REACH)):

        @pl.when(row_parity == parity)
        def _(first=first):
            for index in range(FIELDS):
                far_rows_ref[index * REACH : (index + 1) * REACH, :] = fields_ref[index, first : first + REACH, :]


def strips_from(gy, near_ref, far_ref):
    rows = far_ref.shape[0]
    parity = lax.rem(lax.axis_index(gy), 2)
    near = near_ref[pl.ds(pl.multiple_of((1 - parity) * rows, 8), rows), :]
    far = far_ref[...]
    odd = parity == 1
    return jnp.where(odd, near, far), jnp.where(odd, far, near)


def halo_columns(from_west, from_east, index):
    lane = lane_of(from_west.shape)
    right = pltpu.roll(from_east, (LANES - GAP * index) % LANES, 1)
    left = pltpu.roll(from_west, GAP * index, 1)
    return jnp.where(lane < REACH, right, jnp.where(lane >= LANES - REACH, left, 0.0))


def rows_kernel(gx, gy, fields_ref, near_strip, far_strip, near_ref, corner_ref):
    _, rows, cols = fields_ref.shape
    from_west, from_east = strips_from(gy, near_strip, far_strip)
    parity = lax.rem(lax.axis_index(gx), 2)

    def fill(near_first, far_first):
        for index in range(FIELDS):
            at = slice(index * REACH, (index + 1) * REACH)
            cut = slice(near_first, near_first + REACH)
            near_ref[at, cols : cols + LANES] = halo_columns(from_west[cut], from_east[cut], index)
            near_ref[at, :cols] = fields_ref[index, cut, :]
            cut = slice(far_first, far_first + REACH)
            corner_ref[at, :] = halo_columns(from_west[cut], from_east[cut], index)

    @pl.when(parity == 0)
    def _():
        fill(rows - REACH, 0)

    @pl.when(parity == 1)
    def _():
        fill(0, rows - REACH)


def bessel_weights(duration):
    halved = jnp.full((8, LANES), duration * (SPECTRAL * 0.5), jnp.float32)
    square = -(halved * halved)
    weights = []
    power = jnp.ones((8, LANES), jnp.float32)
    for degree in range(TERMS):
        series = jnp.ones((8, LANES), jnp.float32)
        for counter in range(23, 0, -1):
            series = 1.0 + series * (square * (1.0 / (counter * (counter + degree))))
        scale = (1.0 if degree == 0 else 2.0) / math.factorial(degree)
        weights.append(series * power * scale)
        power = power * halved
    return weights


def main_kernel(gx, gy, copies, duration_ref, fields_ref,
                near_strip, far_strip, near_rows, far_rows, far_corner, out_re, out_im, sums_ref,
                psi, odd, even, total, coeffs, up_left, weight_ref, norm_ref):
    _, rows, cols = fields_ref.shape
    tiles = cols // LANES
    own = PAD + TOP
    scales = (1.0, 1.0, 2.0 / SPECTRAL, -2.0 / SPECTRAL, -2.0 / SPECTRAL)
    targets = [psi.at[0], psi.at[1], coeffs.at[0], coeffs.at[1], coeffs.at[2]]

    for degree, weight in enumerate(bessel_weights(duration_ref[0])):
        weight_ref[degree] = weight

    from_west, from_east = strips_from(gy, near_strip, far_strip)
    for index, (target, scale) in enumerate(zip(targets, scales)):
        for tile in range(tiles + 1):
            if tile == tiles:
                value = halo_columns(from_west, from_east, index)
            else:
                value = fields_ref[index, :, tile * LANES : (tile + 1) * LANES]
            target[tile, own : own + rows, :] = value if scale == 1.0 else value * scale

    packed_rows = far_rows.shape[0]

    def place(from_up, from_down):
        for source, base, start in ((*from_up, own - REACH), (*from_down, own + rows)):
            for index, (target, scale) in enumerate(zip(targets, scales)):
                first = base + index * REACH
                for tile in range(tiles + 1):
                    if tile == tiles and source is far_rows:
                        value = far_corner[first : first + REACH, :]
                    else:
                        value = source[first : first + REACH, tile * LANES : (tile + 1) * LANES]
                    target[tile, start : start + REACH, :] = value if scale == 1.0 else value * scale

    row_parity = lax.rem(lax.axis_index(gx), 2)

    @pl.when(row_parity == 0)
    def _():
        place((far_rows, 0), (near_rows, packed_rows))

    @pl.when(row_parity == 1)
    def _():
        place((near_rows, 0), (far_rows, 0))

    lane = lane_of((8, LANES))
    count = rows // 8
    first_core = TOP // 8
    every = list(range(count + 4))

    def west_of(tile):
        if isinstance(tile, int):
            return (tile - 1) % (tiles + 1)
        return jnp.where(tile == 0, tiles, tile - 1)

    def east_of(tile):
        if isinstance(tile, int):
            return (tile + 1) % (tiles + 1)
        return jnp.where(tile == tiles, 0, tile + 1)

    def shift_coeffs(tile, carry):
        other = west_of(tile)
        for block in every:
            at = pl.ds(PAD + 8 * block, 8)
            up_left[0, tile, at, :] = coeffs[1, tile, pl.ds(PAD + 8 * block - 1, 8), :]
            joined = jnp.where(lane == LANES - 1, coeffs[2, other, at, :], coeffs[2, tile, at, :])
            up_left[1, tile, at, :] = pltpu.roll(joined, 1, 1)
        return carry

    lax.fori_loop(0, tiles + 1, shift_coeffs, 0)

    def apply(step, degree, current, previous, target):
        level = step * (TERMS - 1) + degree
        blocks = [b for b in every
                  if 8 * (b + 1) - TOP > level - REACH and 8 * b - TOP < rows + REACH - level]
        wanted = [b for b in every
                  if 8 * (b + 1) - TOP > -(REACH - TERMS + 1) and 8 * b - TOP < rows + REACH - TERMS + 1]
        core = list(range(first_core, first_core + count))
        last_step = step == STEPS - 1

        def body(tile, carry):
            before, norm, norm_zero = carry
            west, east = west_of(tile), east_of(tile)
            squares = None
            zero_squares = None
            for block in blocks:
                at = pl.ds(PAD + 8 * block, 8)
                pot, hop_d, hop_r = (coeffs[k, tile, at, :] for k in range(3))
                hop_u, hop_l = (up_left[k, tile, at, :] for k in range(2))
                found = []
                for part in range(2):
                    centre = current[part, tile, at, :]
                    below = current[part, tile, pl.ds(PAD + 8 * block + 1, 8), :]
                    above = current[part, tile, pl.ds(PAD + 8 * block - 1, 8), :]
                    left = pltpu.roll(jnp.where(lane == LANES - 1, current[part, west, at, :], centre), 1, 1)
                    right_ = pltpu.roll(jnp.where(lane == 0, current[part, east, at, :], centre), LANES - 1, 1)
                    applied = (pot * centre + hop_d * below) + (hop_u * above + hop_r * right_) + hop_l * left
                    if degree == 1:
                        following = 0.5 * applied
                    else:
                        following = applied - previous[part, tile, at, :]
                    target[part, tile, at, :] = following
                    found.append(following)
                keep = core if last_step else wanted
                if block in keep:
                    quarter = degree % 4
                    first, second = (found[0], found[1]) if quarter % 2 == 0 else (found[1], found[0])
                    weight = weight_ref[degree]
                    adds = (first * weight, second * weight)
                    signs = {0: (1, 1), 1: (1, -1), 2: (-1, -1), 3: (-1, 1)}[quarter]
                    for part in range(2):
                        if degree == 1:
                            base = current[part, tile, at, :] * weight_ref[0]
                        elif last_step:
                            base = even_total[part, tile, pl.ds(PAD + 8 * block, 8), :]
                        else:
                            base = total[part, tile, at, :]
                        value = base + adds[part] if signs[part] > 0 else base - adds[part]
                        if last_step:
                            even_total[part, tile, at, :] = value
                        else:
                            total[part, tile, at, :] = value
                if block in core:
                    for part in range(2):
                        square = found[part] * found[part]
                        squares = square if squares is None else squares + square
                        if degree == 1:
                            start = current[part, tile, at, :]
                            start = start * start
                            zero_squares = start if zero_squares is None else zero_squares + start
            if not isinstance(tile, int):
                squares = jnp.where(tile < tiles, squares, 0.0)
                if degree == 1:
                    zero_squares = jnp.where(tile < tiles, zero_squares, 0.0)
            if not isinstance(tile, int) or tile < tiles:
                norm = norm + squares
                if degree == 1:
                    norm_zero = norm_zero + zero_squares
            return before, norm, norm_zero

        zero = jnp.zeros((8, LANES), jnp.float32)
        carry = (0, zero, zero)
        if UNROLL > tiles:
            for tile in range(tiles + 1):
                carry = body(tile, carry)
        else:
            def group(index, carry):
                for offset in range(UNROLL):
                    carry = body(index * UNROLL + offset, carry)
                return carry

            carry = lax.fori_loop(0, (tiles + 1) // UNROLL, group, carry)
        _, norm, norm_zero = carry
        norm_ref[step * TERMS + degree] = norm
        if degree == 1:
            norm_ref[step * TERMS] = norm_zero

    even_total = psi
    for step in range(STEPS):
        start = psi if step == 0 else total
        sequence = [start, odd, even]
        apply(step, 1, start, None, odd)
        apply(step, 2, odd, start, even)
        for degree in range(3, TERMS):
            if degree % 2:
                apply(step, degree, even, odd, odd)
            else:
                apply(step, degree, odd, even, even)
        source = total if step < STEPS - 1 else even_total
        square = jnp.zeros((8, LANES), jnp.float32)
        for tile in range(tiles):
            for block in range(first_core, first_core + count):
                for part in range(2):
                    value = source[part, tile, pl.ds(PAD + 8 * block, 8), :]
                    square = square + value * value
                    if step == STEPS - 1:
                        out_ref = (out_re, out_im)[part]
                        out_ref[8 * (block - first_core) : 8 * (block - first_core) + 8, tile * LANES : (tile + 1) * LANES] = value
        norm_ref[STEPS * TERMS + step] = square

    lane_row = lane_of((1, LANES))
    packed = jnp.zeros((1, LANES), jnp.float32)
    for index in range(STEPS * TERMS + STEPS):
        found = jnp.sum(jnp.sum(norm_ref[index], axis=0, keepdims=True), axis=1, keepdims=True)
        packed = jnp.where(lane_row == index, found, packed)
    sums_ref[...] = jnp.broadcast_to(packed, (copies, LANES))


def scale_kernel(cell_count, totals_ref, re_ref, im_ref, out_re, out_im, norms_ref):
    totals = jnp.sum(totals_ref[...], axis=0, keepdims=True) * (1.0 / cell_count)
    lane = lane_of(totals.shape)
    factor = jnp.ones((1, 1), jnp.float32)
    for step in range(STEPS):
        squared = factor * factor
        moved = totals if step == 0 else pltpu.roll(totals, LANES - step * TERMS, 1)
        norms_ref[step] = (moved * squared)[:, :TERMS]
        mean = jnp.sum(jnp.where(lane == STEPS * TERMS + step, totals, 0.0), axis=1, keepdims=True) * squared
        factor = factor * lax.rsqrt(mean + EPSILON)
    out_re[0] = re_ref[...] * factor
    out_im[0] = im_ref[...] * factor


def far_pairs(count):
    pairs = [(i, (i + 1) % count) for i in range(1, count, 2)]
    return pairs + [(target, source) for source, target in pairs]


def near_pairs(count):
    return [[i, i + 1] for i in range(0, count, 2)]


def from_far_one(value, axis, count):
    return lax.ppermute(value, axis, far_pairs(count))


def from_near_one(value, axis, count):
    return lax.all_gather(value, axis, axis=0, tiled=True, axis_index_groups=near_pairs(count))


FIELDS_PARAMS = pltpu.CompilerParams(vmem_limit_bytes=20 * 2**20)


def grant(mebibytes):
    return pltpu.CompilerParams(vmem_limit_bytes=mebibytes * 2**20)


def vmem_specs(count):
    return [pl.BlockSpec(memory_space=VMEM)] * count


def per_device(gx, gy, counts, init_re, init_im, onsite, bond_x, bond_y, hop_table, centre, duration):
    rows, cols = onsite.shape
    extents = (rows * counts[0], cols * counts[1])
    tiles = cols // LANES
    chips = counts[0] * counts[1] // 2
    smem = [pl.BlockSpec(memory_space=SMEM)]
    local = (init_re, init_im, onsite, bond_x, bond_y)
    shape = lambda *s: jax.ShapeDtypeStruct(s, jnp.float32)
    height = rows + 2 * TOP + 2 * PAD

    hbm = [pl.BlockSpec(memory_space=pltpu.HBM)]
    packed_rows = -(-FIELDS * REACH // 8) * 8
    fields, near, far, far_main = pl.pallas_call(
        functools.partial(fields_kernel, gx, gy, extents),
        out_shape=[shape(FIELDS, rows, cols), shape(rows, LANES), shape(rows, LANES), shape(packed_rows, cols)],
        in_specs=hbm * 7, out_specs=vmem_specs(4),
        scratch_shapes=[SMEM(hop_table.shape, jnp.float32), SMEM(centre.shape, jnp.int32), VMEM((2, rows, cols), jnp.float32),
                        VMEM((2, rows, cols), jnp.int32), pltpu.SemaphoreType.DMA((7,))],
        name="fields", compiler_params=FIELDS_PARAMS,
    )(*(pltpu.with_memory_space_constraint(x, pltpu.HBM) for x in (hop_table, centre, *local)))
    far_rows = from_far_one(far_main, gx, counts[0])
    far_strip = from_far_one(far, gy[0], counts[1])
    near_strip = from_near_one(near, gy[0], counts[1])
    near, corner = pl.pallas_call(
        functools.partial(rows_kernel, gx, gy),
        out_shape=[shape(packed_rows, cols + LANES), shape(packed_rows, LANES)],
        in_specs=vmem_specs(3), out_specs=vmem_specs(2), name="rows", compiler_params=grant(8),
    )(fields, near_strip, far_strip)
    far_corner = from_far_one(corner, gx, counts[0])
    near_rows = from_near_one(near, gx, counts[0])
    panel = lambda n: pltpu.VMEM((n, tiles + 1, height, LANES), jnp.float32)
    acc_re, acc_im, sums = pl.pallas_call(
        functools.partial(main_kernel, gx, gy, chips),
        out_shape=[shape(rows, cols), shape(rows, cols), shape(chips, LANES)],
        in_specs=smem + vmem_specs(6), out_specs=vmem_specs(3),
        scratch_shapes=[panel(2), panel(2), panel(2), panel(2), panel(3), panel(2),
                        pltpu.VMEM((TERMS, 8, LANES), jnp.float32),
                        pltpu.VMEM((STEPS * TERMS + STEPS, 8, LANES), jnp.float32)],
        name="chebyshev", compiler_params=grant(20),
    )(duration, fields, near_strip, far_strip, near_rows, far_rows, far_corner)
    sums = lax.all_gather(sums, gx[1], axis=0, tiled=True)
    sums = sums[:chips] + sums[chips:]
    totals = lax.all_to_all(sums, (gx[0], *gy), 0, 0, tiled=True)
    out_re, out_im, norms = pl.pallas_call(
        functools.partial(scale_kernel, extents[0] * extents[1]),
        out_shape=[shape(1, rows, cols), shape(1, rows, cols), shape(STEPS, 1, TERMS)],
        in_specs=vmem_specs(3), out_specs=vmem_specs(3), name="scale", compiler_params=grant(4),
    )(totals, acc_re, acc_im)
    return out_re, out_im, jnp.swapaxes(norms, 1, 2)


def solution(mesh):
    counts = (mesh.shape["gx"], mesh.shape["gy"])
    finer = Mesh(mesh.devices.reshape(counts[0] // 2, 2, counts[1]), ("chip", "core", "gy"))
    gx, gy = ("chip", "core"), ("gy",)
    whole, plane = P(None, gx, "gy"), P(gx, "gy")
    return jax.shard_map(
        functools.partial(per_device, gx, gy, counts),
        mesh=finer,
        in_specs=(whole, whole, plane, plane, plane, P(), P(), P()),
        out_specs=(whole, whole, P()),
        check_vma=False,
    )
```

```python
import functools
import math

import jax
import jax.numpy as jnp
from jax import lax
from jax.experimental import pallas as pl
from jax.experimental.pallas import tpu as pltpu
from jax.sharding import Mesh
from jax.sharding import PartitionSpec as P

TERMS = 8
STEPS = 2
SPECTRAL = 7.5
EPSILON = 1e-06
REACH = STEPS * (TERMS - 1)
LANES = 128
GAP = 16
PAD = 8
TOP = 16
FIELDS = 5
UNROLL = 9
VMEM = pltpu.VMEM
SMEM = pltpu.SMEM


def lane_of(shape):
    return lax.broadcasted_iota(jnp.int32, shape, len(shape) - 1)


def falloff(positions, centre, extent):
    distance = positions - centre
    distance = jnp.where(distance < 0, distance + extent, distance)
    distance = jnp.minimum(distance, extent - distance).astype(jnp.float32)
    return jnp.exp(-(distance * distance * (4.5 / (extent * extent))))


def row_envelope(start, count, row_base, centre, extent):
    positions = row_base + start + lax.broadcasted_iota(jnp.int32, (count, LANES), 0)
    return falloff(positions, centre, extent)


def column_envelope(tile, column_base, centre, extent):
    positions = column_base + tile * LANES + lane_of((1, LANES))
    return falloff(positions, centre, extent)


def table_lanes(table_ref, classes):
    lane = lane_of((8, LANES))
    table = jnp.zeros((8, LANES), jnp.float32)
    for entry in range(classes):
        table = jnp.where(lane == entry, table_ref[entry], table)
    return table


def looked_up(table, codes):
    rows = codes.shape[0]
    whole = jnp.concatenate([table] * -(-rows // 8), axis=0)[:rows]
    return jnp.take_along_axis(whole, codes, axis=1)


def bases(rows, cols, gx, gy):
    return lax.axis_index(gx) * rows, lax.axis_index(gy) * cols


def fields_kernel(gx, gy, extents, table_hbm, centre_hbm, re, im, onsite, down, right, fields_ref, near_ref, far_ref, far_rows_ref,
                  table_ref, centre_ref, fine, codes, sems):
    rows, cols = onsite.shape
    copies = [
        (table_hbm, table_ref),
        (centre_hbm, centre_ref),
        (re.at[0], fine.at[0]),
        (im.at[0], fine.at[1]),
        (down, codes.at[0]),
        (right, codes.at[1]),
        (onsite, fields_ref.at[2]),
    ]
    started = [pltpu.make_async_copy(source, target, sems.at[i]) for i, (source, target) in enumerate(copies)]
    for copy in started:
        copy.start()
    for copy in started:
        copy.wait()
    row_base, col_base = bases(rows, cols, gx, gy)
    table = table_lanes(table_ref, table_ref.shape[0])
    row_part = row_envelope(0, rows, row_base, centre_ref[0, 0], extents[0])
    lane = lane_of((rows, LANES))
    tiles = cols // LANES
    packs = []
    for tile in (0, tiles - 1, *range(1, tiles - 1)):
        cut = slice(tile * LANES, (tile + 1) * LANES)
        envelope = row_part * column_envelope(tile, col_base, centre_ref[0, 1], extents[1])
        values = [
            fine[0, :, cut] * envelope,
            fine[1, :, cut] * envelope,
            fields_ref[2, :, cut],
            looked_up(table, codes[0, :, cut]),
            looked_up(table, codes[1, :, cut]),
        ]
        for index in (0, 1, 3, 4):
            fields_ref[index, :, cut] = values[index]
        if 0 < tile < tiles - 1:
            continue
        packed = jnp.zeros((rows, LANES), jnp.float32)
        for index, value in enumerate(values):
            if tile:
                moved = pltpu.roll(value, (LANES - GAP * index) % LANES, 1)
                inside = (lane >= LANES - REACH - GAP * index) & (lane < LANES - GAP * index)
            else:
                moved = pltpu.roll(value, GAP * index, 1)
                inside = (lane >= GAP * index) & (lane < GAP * index + REACH)
            packed = jnp.where(inside, moved, packed)
        packs.append(packed)
    west, east = packs
    odd = lax.rem(lax.axis_index(gy), 2) == 1
    near_ref[...] = jnp.where(odd, west, east)
    far_ref[...] = jnp.where(odd, east, west)
    row_parity = lax.rem(lax.axis_index(gx), 2)
    for parity, first in ((0, 0), (1, rows - REACH)):

        @pl.when(row_parity == parity)
        def _(first=first):
            for index in range(FIELDS):
                far_rows_ref[index * REACH : (index + 1) * REACH, :] = fields_ref[index, first : first + REACH, :]


def strips_from(gy, near_ref, far_ref):
    rows = far_ref.shape[0]
    parity = lax.rem(lax.axis_index(gy), 2)
    near = near_ref[pl.ds(pl.multiple_of((1 - parity) * rows, 8), rows), :]
    far = far_ref[...]
    odd = parity == 1
    return jnp.where(odd, near, far), jnp.where(odd, far, near)


def halo_columns(from_west, from_east, index):
    lane = lane_of(from_west.shape)
    right = pltpu.roll(from_east, (LANES - GAP * index) % LANES, 1)
    left = pltpu.roll(from_west, GAP * index, 1)
    return jnp.where(lane < REACH, right, jnp.where(lane >= LANES - REACH, left, 0.0))


def rows_kernel(gx, gy, fields_ref, near_strip, far_strip, near_ref, corner_ref):
    _, rows, cols = fields_ref.shape
    from_west, from_east = strips_from(gy, near_strip, far_strip)
    parity = lax.rem(lax.axis_index(gx), 2)

    def fill(near_first, far_first):
        for index in range(FIELDS):
            at = slice(index * REACH, (index + 1) * REACH)
            cut = slice(near_first, near_first + REACH)
            near_ref[at, cols : cols + LANES] = halo_columns(from_west[cut], from_east[cut], index)
            near_ref[at, :cols] = fields_ref[index, cut, :]
            cut = slice(far_first, far_first + REACH)
            corner_ref[at, :] = halo_columns(from_west[cut], from_east[cut], index)

    @pl.when(parity == 0)
    def _():
        fill(rows - REACH, 0)

    @pl.when(parity == 1)
    def _():
        fill(0, rows - REACH)


def bessel_weights(duration):
    halved = jnp.full((8, LANES), duration * (SPECTRAL * 0.5), jnp.float32)
    square = -(halved * halved)
    weights = []
    power = jnp.ones((8, LANES), jnp.float32)
    for degree in range(TERMS):
        series = jnp.ones((8, LANES), jnp.float32)
        for counter in range(23, 0, -1):
            series = 1.0 + series * (square * (1.0 / (counter * (counter + degree))))
        scale = (1.0 if degree == 0 else 2.0) / math.factorial(degree)
        weights.append(series * power * scale)
        power = power * halved
    return weights


def main_kernel(gx, gy, copies, duration_ref, fields_ref,
                near_strip, far_strip, near_rows, far_rows, far_corner, out_re, out_im, sums_ref,
                psi, odd, even, total, coeffs, up_left, weight_ref, norm_ref):
    _, rows, cols = fields_ref.shape
    tiles = cols // LANES
    own = PAD + TOP
    scales = (1.0, 1.0, 2.0 / SPECTRAL, -2.0 / SPECTRAL, -2.0 / SPECTRAL)
    targets = [psi.at[0], psi.at[1], coeffs.at[0], coeffs.at[1], coeffs.at[2]]

    for degree, weight in enumerate(bessel_weights(duration_ref[0])):
        weight_ref[degree] = weight

    from_west, from_east = strips_from(gy, near_strip, far_strip)
    for index, (target, scale) in enumerate(zip(targets, scales)):
        for tile in range(tiles + 1):
            if tile == tiles:
                value = halo_columns(from_west, from_east, index)
            else:
                value = fields_ref[index, :, tile * LANES : (tile + 1) * LANES]
            target[tile, own : own + rows, :] = value if scale == 1.0 else value * scale

    packed_rows = far_rows.shape[0]

    def place(from_up, from_down):
        for source, base, start in ((*from_up, own - REACH), (*from_down, own + rows)):
            for index, (target, scale) in enumerate(zip(targets, scales)):
                first = base + index * REACH
                for tile in range(tiles + 1):
                    if tile == tiles and source is far_rows:
                        value = far_corner[first : first + REACH, :]
                    else:
                        value = source[first : first + REACH, tile * LANES : (tile + 1) * LANES]
                    target[tile, start : start + REACH, :] = value if scale == 1.0 else value * scale

    row_parity = lax.rem(lax.axis_index(gx), 2)

    @pl.when(row_parity == 0)
    def _():
        place((far_rows, 0), (near_rows, packed_rows))

    @pl.when(row_parity == 1)
    def _():
        place((near_rows, 0), (far_rows, 0))

    lane = lane_of((8, LANES))
    count = rows // 8
    first_core = TOP // 8
    every = list(range(count + 4))

    def west_of(tile):
        if isinstance(tile, int):
            return (tile - 1) % (tiles + 1)
        return jnp.where(tile == 0, tiles, tile - 1)

    def east_of(tile):
        if isinstance(tile, int):
            return (tile + 1) % (tiles + 1)
        return jnp.where(tile == tiles, 0, tile + 1)

    def shift_coeffs(tile, carry):
        other = west_of(tile)
        for block in every:
            at = pl.ds(PAD + 8 * block, 8)
            up_left[0, tile, at, :] = coeffs[1, tile, pl.ds(PAD + 8 * block - 1, 8), :]
            joined = jnp.where(lane == LANES - 1, coeffs[2, other, at, :], coeffs[2, tile, at, :])
            up_left[1, tile, at, :] = pltpu.roll(joined, 1, 1)
        return carry

    for tile in range(tiles + 1):
        shift_coeffs(tile, 0)

    def apply(step, degree, current, previous, target):
        level = step * (TERMS - 1) + degree
        blocks = [b for b in every
                  if 8 * (b + 1) - TOP > level - REACH and 8 * b - TOP < rows + REACH - level]
        wanted = [b for b in every
                  if 8 * (b + 1) - TOP > -(REACH - TERMS + 1) and 8 * b - TOP < rows + REACH - TERMS + 1]
        core = list(range(first_core, first_core + count))
        last_step = step == STEPS - 1

        def body(tile, carry):
            before, norm, norm_zero = carry
            west, east = west_of(tile), east_of(tile)
            squares = None
            zero_squares = None
            for block in blocks:
                at = pl.ds(PAD + 8 * block, 8)
                pot, hop_d, hop_r = (coeffs[k, tile, at, :] for k in range(3))
                hop_u, hop_l = (up_left[k, tile, at, :] for k in range(2))
                found = []
                for part in range(2):
                    centre = current[part, tile, at, :]
                    below = current[part, tile, pl.ds(PAD + 8 * block + 1, 8), :]
                    above = current[part, tile, pl.ds(PAD + 8 * block - 1, 8), :]
                    left = pltpu.roll(jnp.where(lane == LANES - 1, current[part, west, at, :], centre), 1, 1)
                    right_ = pltpu.roll(jnp.where(lane == 0, current[part, east, at, :], centre), LANES - 1, 1)
                    applied = (pot * centre + hop_d * below) + (hop_u * above + hop_r * right_) + hop_l * left
                    if degree == 1:
                        following = 0.5 * applied
                    else:
                        following = applied - previous[part, tile, at, :]
                    target[part, tile, at, :] = following
                    found.append(following)
                keep = core if last_step else wanted
                if block in keep:
                    quarter = degree % 4
                    first, second = (found[0], found[1]) if quarter % 2 == 0 else (found[1], found[0])
                    weight = weight_ref[degree]
                    adds = (first * weight, second * weight)
                    signs = {0: (1, 1), 1: (1, -1), 2: (-1, -1), 3: (-1, 1)}[quarter]
                    for part in range(2):
                        if degree == 1:
                            base = current[part, tile, at, :] * weight_ref[0]
                        elif last_step:
                            base = even_total[part, tile, pl.ds(PAD + 8 * block, 8), :]
                        else:
                            base = total[part, tile, at, :]
                        value = base + adds[part] if signs[part] > 0 else base - adds[part]
                        if last_step:
                            even_total[part, tile, at, :] = value
                        else:
                            total[part, tile, at, :] = value
                if block in core:
                    for part in range(2):
                        square = found[part] * found[part]
                        squares = square if squares is None else squares + square
                        if degree == 1:
                            start = current[part, tile, at, :]
                            start = start * start
                            zero_squares = start if zero_squares is None else zero_squares + start
            if not isinstance(tile, int):
                squares = jnp.where(tile < tiles, squares, 0.0)
                if degree == 1:
                    zero_squares = jnp.where(tile < tiles, zero_squares, 0.0)
            if not isinstance(tile, int) or tile < tiles:
                norm = norm + squares
                if degree == 1:
                    norm_zero = norm_zero + zero_squares
            return before, norm, norm_zero

        zero = jnp.zeros((8, LANES), jnp.float32)
        carry = (0, zero, zero)
        if UNROLL > tiles:
            for tile in range(tiles + 1):
                carry = body(tile, carry)
        else:
            def group(index, carry):
                for offset in range(UNROLL):
                    carry = body(index * UNROLL + offset, carry)
                return carry

            carry = lax.fori_loop(0, (tiles + 1) // UNROLL, group, carry)
        _, norm, norm_zero = carry
        norm_ref[step * TERMS + degree] = norm
        if degree == 1:
            norm_ref[step * TERMS] = norm_zero

    even_total = psi
    for step in range(STEPS):
        start = psi if step == 0 else total
        sequence = [start, odd, even]
        apply(step, 1, start, None, odd)
        apply(step, 2, odd, start, even)
        for degree in range(3, TERMS):
            if degree % 2:
                apply(step, degree, even, odd, odd)
            else:
                apply(step, degree, odd, even, even)
        source = total if step < STEPS - 1 else even_total
        square = jnp.zeros((8, LANES), jnp.float32)
        for tile in range(tiles):
            for block in range(first_core, first_core + count):
                for part in range(2):
                    value = source[part, tile, pl.ds(PAD + 8 * block, 8), :]
                    square = square + value * value
                    if step == STEPS - 1:
                        out_ref = (out_re, out_im)[part]
                        out_ref[8 * (block - first_core) : 8 * (block - first_core) + 8, tile * LANES : (tile + 1) * LANES] = value
        norm_ref[STEPS * TERMS + step] = square

    lane_row = lane_of((1, LANES))
    packed = jnp.zeros((1, LANES), jnp.float32)
    for index in range(STEPS * TERMS + STEPS):
        found = jnp.sum(jnp.sum(norm_ref[index], axis=0, keepdims=True), axis=1, keepdims=True)
        packed = jnp.where(lane_row == index, found, packed)
    sums_ref[...] = jnp.broadcast_to(packed, (copies, LANES))


def scale_kernel(cell_count, totals_ref, re_ref, im_ref, out_re, out_im, norms_ref):
    totals = jnp.sum(totals_ref[...], axis=0, keepdims=True) * (1.0 / cell_count)
    lane = lane_of(totals.shape)
    factor = jnp.ones((1, 1), jnp.float32)
    for step in range(STEPS):
        squared = factor * factor
        moved = totals if step == 0 else pltpu.roll(totals, LANES - step * TERMS, 1)
        norms_ref[step] = (moved * squared)[:, :TERMS]
        mean = jnp.sum(jnp.where(lane == STEPS * TERMS + step, totals, 0.0), axis=1, keepdims=True) * squared
        factor = factor * lax.rsqrt(mean + EPSILON)
    out_re[0] = re_ref[...] * factor
    out_im[0] = im_ref[...] * factor


def far_pairs(count):
    pairs = [(i, (i + 1) % count) for i in range(1, count, 2)]
    return pairs + [(target, source) for source, target in pairs]


def near_pairs(count):
    return [[i, i + 1] for i in range(0, count, 2)]


def from_far_one(value, axis, count):
    return lax.ppermute(value, axis, far_pairs(count))


def from_near_one(value, axis, count):
    return lax.all_gather(value, axis, axis=0, tiled=True, axis_index_groups=near_pairs(count))


FIELDS_PARAMS = pltpu.CompilerParams(vmem_limit_bytes=20 * 2**20)


def grant(mebibytes):
    return pltpu.CompilerParams(vmem_limit_bytes=mebibytes * 2**20)


def vmem_specs(count):
    return [pl.BlockSpec(memory_space=VMEM)] * count


def per_device(gx, gy, counts, init_re, init_im, onsite, bond_x, bond_y, hop_table, centre, duration):
    rows, cols = onsite.shape
    extents = (rows * counts[0], cols * counts[1])
    tiles = cols // LANES
    chips = counts[0] * counts[1] // 2
    smem = [pl.BlockSpec(memory_space=SMEM)]
    local = (init_re, init_im, onsite, bond_x, bond_y)
    shape = lambda *s: jax.ShapeDtypeStruct(s, jnp.float32)
    height = rows + 2 * TOP + 2 * PAD

    hbm = [pl.BlockSpec(memory_space=pltpu.HBM)]
    packed_rows = -(-FIELDS * REACH // 8) * 8
    fields, near, far, far_main = pl.pallas_call(
        functools.partial(fields_kernel, gx, gy, extents),
        out_shape=[shape(FIELDS, rows, cols), shape(rows, LANES), shape(rows, LANES), shape(packed_rows, cols)],
        in_specs=hbm * 7, out_specs=vmem_specs(4),
        scratch_shapes=[SMEM(hop_table.shape, jnp.float32), SMEM(centre.shape, jnp.int32), VMEM((2, rows, cols), jnp.float32),
                        VMEM((2, rows, cols), jnp.int32), pltpu.SemaphoreType.DMA((7,))],
        name="fields", compiler_params=FIELDS_PARAMS,
    )(*(pltpu.with_memory_space_constraint(x, pltpu.HBM) for x in (hop_table, centre, *local)))
    far_rows = from_far_one(far_main, gx, counts[0])
    far_strip = from_far_one(far, gy[0], counts[1])
    near_strip = from_near_one(near, gy[0], counts[1])
    near, corner = pl.pallas_call(
        functools.partial(rows_kernel, gx, gy),
        out_shape=[shape(packed_rows, cols + LANES), shape(packed_rows, LANES)],
        in_specs=vmem_specs(3), out_specs=vmem_specs(2), name="rows", compiler_params=grant(8),
    )(fields, near_strip, far_strip)
    far_corner = from_far_one(corner, gx, counts[0])
    near_rows = from_near_one(near, gx, counts[0])
    panel = lambda n: pltpu.VMEM((n, tiles + 1, height, LANES), jnp.float32)
    acc_re, acc_im, sums = pl.pallas_call(
        functools.partial(main_kernel, gx, gy, chips),
        out_shape=[shape(rows, cols), shape(rows, cols), shape(chips, LANES)],
        in_specs=smem + vmem_specs(6), out_specs=vmem_specs(3),
        scratch_shapes=[panel(2), panel(2), panel(2), panel(2), panel(3), panel(2),
                        pltpu.VMEM((TERMS, 8, LANES), jnp.float32),
                        pltpu.VMEM((STEPS * TERMS + STEPS, 8, LANES), jnp.float32)],
        name="chebyshev", compiler_params=grant(20),
    )(duration, fields, near_strip, far_strip, near_rows, far_rows, far_corner)
    sums = lax.all_gather(sums, gx[1], axis=0, tiled=True)
    sums = sums[:chips] + sums[chips:]
    totals = lax.all_to_all(sums, (gx[0], *gy), 0, 0, tiled=True)
    out_re, out_im, norms = pl.pallas_call(
        functools.partial(scale_kernel, extents[0] * extents[1]),
        out_shape=[shape(1, rows, cols), shape(1, rows, cols), shape(STEPS, 1, TERMS)],
        in_specs=vmem_specs(3), out_specs=vmem_specs(3), name="scale", compiler_params=grant(4),
    )(totals, acc_re, acc_im)
    return out_re, out_im, jnp.swapaxes(norms, 1, 2)


def solution(mesh):
    counts = (mesh.shape["gx"], mesh.shape["gy"])
    finer = Mesh(mesh.devices.reshape(counts[0] // 2, 2, counts[1]), ("chip", "core", "gy"))
    gx, gy = ("chip", "core"), ("gy",)
    whole, plane = P(None, gx, "gy"), P(gx, "gy")
    return jax.shard_map(
        functools.partial(per_device, gx, gy, counts),
        mesh=finer,
        in_specs=(whole, whole, plane, plane, plane, P(), P(), P()),
        out_specs=(whole, whole, P()),
        check_vma=False,
    )
```
